32 devices in a mesh: dp: 8 (over y, x, core), tensor: 4 (over z).
Axes of the slice: x: 2, y: 2, z: 4, core: 2. Of those that a mesh axis runs over, the one named last changes fastest.
Arguments:
- hidden_states: float32 [4096, 2048], P(('dp', 'tensor')), may hold values from -40 to 40
- lengths: int32 [8], P('dp'), may hold values from 128 to 512
- shard_order: int32 [8], replicated, may hold values from 0 to 7, each once
- gain_attn: float32 [2048], replicated, may hold values from 0.25 to 1.75
- w_query: bfloat16 [2048, 2048], P('dp', 'tensor'), may hold values from -0.015625 to 0.015625
- w_key: bfloat16 [2048, 2048], P('dp', 'tensor'), may hold values from -0.125 to 0.125
- w_value: bfloat16 [2048, 2048], P('dp', 'tensor'), may hold values from -0.125 to 0.125
- w_out: bfloat16 [2048, 2048], P('tensor', 'dp'), may hold values from -1 to 1
- rel_bias: float32 [32, 32], P(None, 'tensor'), may hold values from -6 to 300
- gain_ff: float32 [2048], replicated, may hold values from 0.25 to 1.75
- w_gate: bfloat16 [2048, 5120], P('dp', 'tensor'), may hold values from -0.125 to 0.125
- w_up: bfloat16 [2048, 5120], P('dp', 'tensor'), may hold values from -0.125 to 0.125
- w_down: bfloat16 [5120, 2048], P('tensor', 'dp'), may hold values from -0.078125 to 0.078125
- gain_final: float32 [2048], replicated, may hold values from 0.25 to 1.75
- w_reward: float32 [2048], replicated, may hold values from -0.125 to 0.125
Outputs:
- layer_output: float32 [4096, 2048], P(('dp', 'tensor'))
- normalized_rewards: float32 [8], P('dp')
The draws below stay inside these ranges and needn't reach their ends.
Inputs may be any that keep to these rules, and one draw needn't show every extreme that they name: `shard_order`: each of 0 to 8 - 1 appears once. `lengths`: positions at or beyond a rollout's length are padding.
All inputs are finite; a program needn't handle non-finite values.
Results may differ from the reference program's by a relative error of at most 0.02.
Values may be sent and summed in bfloat16 or wider, within the bound.
No kernel may reach another device: no remote copies, remote signals or barrier semaphores. Data moves between devices by JAX's collectives and lax.ppermute only.
A program may use at most 128 MiB of HBM per device.

```python
import math
import jax
import jax.numpy as jnp
from jax import lax

D = 2048
HEADS = 32
DK = 64
FF = 5120
BUCKETS = 32
LEN = 512
SEQS = 8
TOKENS = 4096
N_DP = 8
N_TENSOR = 4


def draw_hidden_states(key, part):
    subkeys = jax.random.split(key, 3)
    base_draw = jnp.clip(jax.random.normal(subkeys[0], (TOKENS, D), jnp.float32), -4.0, 4.0)
    row_scale = jnp.exp(jax.random.uniform(subkeys[1], (TOKENS, 1), jnp.float32, math.log(0.3), math.log(3.0)))
    column_scale = jnp.exp(jax.random.uniform(subkeys[2], (1, D), jnp.float32, math.log(0.3), math.log(3.0)))
    return base_draw * row_scale * column_scale


def draw_rel_bias(key, part):
    subkeys = jax.random.split(key, 1)
    base_draw = jnp.clip(jax.random.normal(subkeys[0], (BUCKETS, HEADS), jnp.float32), -6.0, 6.0)
    return base_draw


def touch_ends(drawn, own_key, smallest, high):
    shape = drawn.shape
    place = [jax.random.randint(jax.random.fold_in(own_key, axis), (), 0, shape[axis]) for axis in range(len(shape))]
    drawn = drawn.at[tuple(place)].set(smallest)
    longest = shape.index(max(shape))
    place[longest] = (place[longest] + 1) % shape[longest]
    return drawn.at[tuple(place)].set(high)


def shard_levels(own_key, shape, cuts, low, largest):
    def one(position, blocks):
        steps = jax.random.uniform(jax.random.fold_in(jax.random.fold_in(own_key, 6), position), (blocks,), jnp.float32, low / len(cuts), largest / len(cuts))
        return jnp.repeat(jnp.exp(steps), shape[position] // blocks).reshape((-1,) + (1,) * (len(shape) - position - 1))

    gain = one(*cuts[0])
    for cut in cuts[1:]:
        gain = gain * one(*cut)
    return gain


def centred(rng, dims, scale, bound, pieces=(), held_as=jnp.bfloat16):
    loudness = shard_levels(rng, dims, pieces, -0.22, 0.18) if pieces else 1.0
    drawn = jax.random.normal(rng, dims, jnp.float32) * scale * loudness
    return jnp.minimum(jnp.maximum(drawn, -bound), bound).astype(held_as)


def setup_inputs(seed: int = 0) -> dict:
    arg_keys = jax.random.split(jax.random.key(seed), 16)
    return {
        "hidden_states": draw_hidden_states(jax.random.fold_in(arg_keys[15], 71), 0),
        "lengths": touch_ends(jax.random.randint(arg_keys[1], (SEQS,), LEN // 4, LEN + 1), jax.random.fold_in(arg_keys[1], 1), LEN // 4, LEN).astype(jnp.int32),
        "shard_order": jax.random.permutation(arg_keys[2], N_DP).astype(jnp.int32),
        "gain_attn": jnp.clip(1.0 + 0.15 * jax.random.normal(arg_keys[3], (D,), jnp.float32), 0.25, 1.75),
        "w_query": centred(arg_keys[4], (D, HEADS * DK), (D * DK) ** -0.5, 0.015625, ((0, 8), (1, 4))),
        "w_key": centred(arg_keys[5], (D, HEADS * DK), D ** -0.5, 0.125, ((0, 8), (1, 4))),
        "w_value": centred(arg_keys[6], (D, HEADS * DK), D ** -0.5, 0.125, ((0, 8), (1, 4))),
        "w_out": centred(arg_keys[7], (HEADS * DK, D), (HEADS * DK // 64) ** -0.5, 1.0, ((0, 4), (1, 8))),
        "rel_bias": draw_rel_bias(jax.random.fold_in(arg_keys[15], 71), 0),
        "gain_ff": jnp.clip(1.0 + 0.15 * jax.random.normal(arg_keys[9], (D,), jnp.float32), 0.25, 1.75),
        "w_gate": centred(arg_keys[10], (D, FF), D ** -0.5, 0.125, ((0, 8), (1, 4))),
        "w_up": centred(arg_keys[11], (D, FF), D ** -0.5, 0.125, ((0, 8), (1, 4))),
        "w_down": centred(arg_keys[12], (FF, D), FF ** -0.5, 0.078125, ((0, 4), (1, 8))),
        "gain_final": jnp.clip(1.0 + 0.15 * jax.random.normal(arg_keys[13], (D,), jnp.float32), 0.25, 1.75),
        "w_reward": centred(arg_keys[14], (D,), D ** -0.5, 0.125, (), jnp.float32),
    }


bucket_edges = (12, 16, 23, 32, 46, 64, 91)

def bucket_index(relative):
    distance = jnp.abs(relative)
    bucket_low = jnp.minimum(distance, 8)
    for threshold in bucket_edges:
        bucket_low = bucket_low + (distance >= threshold).astype(jnp.int32)
    return (jnp.where(relative > 0, 16, 0) + bucket_low).astype(jnp.int32)

def rms_norm(values_in, weight_gain):
    return values_in * lax.rsqrt(lax.optimization_barrier(jnp.mean(values_in * values_in, axis=-1, keepdims=True)) + 1e-06) * weight_gain

def restore_rows(matrix, inverse):
    blocks = matrix.reshape(N_DP, matrix.shape[0] // N_DP, matrix.shape[1])
    return jnp.take(blocks, inverse, axis=0).reshape(matrix.shape)

def restore_columns(matrix, inverse):
    blocks = matrix.reshape(matrix.shape[0], N_DP, matrix.shape[1] // N_DP)
    return jnp.take(blocks, inverse, axis=1).reshape(matrix.shape)

def group_sum(left, right):
    inner = left.shape[1] // N_TENSOR
    left_groups = left.reshape(left.shape[0], N_TENSOR, inner).astype(jnp.float32)
    right_groups = right.reshape(N_TENSOR, inner, right.shape[1]).astype(jnp.float32)
    partials = jnp.einsum('ljc,jcd->jld', left_groups, right_groups).astype(jnp.bfloat16)
    partials = lax.optimization_barrier(partials)
    return lax.optimization_barrier(jnp.sum(partials.astype(jnp.float32), axis=0))

def reference(hidden_states, lengths, shard_order, gain_attn, w_query, w_key, w_value, w_out, rel_bias, gain_ff, w_gate, w_up, w_down, gain_final, w_reward):
    inverse = jnp.argsort(shard_order).astype(jnp.int32)
    query_true = restore_rows(w_query, inverse)
    key_true = restore_rows(w_key, inverse)
    value_true = restore_rows(w_value, inverse)
    gate_true = restore_rows(w_gate, inverse)
    up_true = restore_rows(w_up, inverse)
    out_true = restore_columns(w_out, inverse)
    down_true = restore_columns(w_down, inverse)
    positions = jnp.arange(LEN, dtype=jnp.int32)
    relative = positions[None, :] - positions[:, None]
    position_bias = jnp.transpose(rel_bias[bucket_index(relative)], (2, 0, 1))

    def sequence_step(operands):
        states, length = operands
        normed = rms_norm(states, gain_attn).astype(jnp.bfloat16)
        queries = jnp.dot(normed, query_true, preferred_element_type=jnp.float32).astype(jnp.bfloat16)
        key_states = jnp.dot(normed, key_true, preferred_element_type=jnp.float32).astype(jnp.bfloat16)
        value_states = jnp.dot(normed, value_true, preferred_element_type=jnp.float32).astype(jnp.bfloat16)
        query_heads = queries.reshape(LEN, HEADS, DK).astype(jnp.float32)
        key_heads = key_states.reshape(LEN, HEADS, DK).astype(jnp.float32)
        value_heads = value_states.reshape(LEN, HEADS, DK).astype(jnp.float32)
        scores = jnp.einsum('qhd,khd->hqk', query_heads, key_heads) + position_bias
        in_range = positions < length
        scores = jnp.where(in_range[None, None, :], scores, -1e+30)
        row_max = lax.optimization_barrier(jnp.max(scores, axis=-1, keepdims=True))
        exp_scores = jnp.exp(scores - row_max)
        soft_weights = (exp_scores / lax.optimization_barrier(jnp.sum(exp_scores, axis=-1, keepdims=True))).astype(jnp.bfloat16)
        context = jnp.einsum('hqk,khd->qhd', soft_weights.astype(jnp.float32), value_heads)
        context = context.astype(jnp.bfloat16).reshape(LEN, HEADS * DK)
        mid = states + group_sum(context, out_true)
        mid_normed = rms_norm(mid, gain_ff).astype(jnp.bfloat16)
        gate_proj = jnp.dot(mid_normed, gate_true, preferred_element_type=jnp.float32)
        up_proj = jnp.dot(mid_normed, up_true, preferred_element_type=jnp.float32)
        activated = (jax.nn.gelu(gate_proj, approximate=True) * up_proj).astype(jnp.bfloat16)
        layer_output = mid + group_sum(activated, down_true)
        final_normed = rms_norm(layer_output, gain_final)
        token_score = jnp.dot(final_normed, w_reward, precision=lax.Precision.HIGHEST)
        pooled_sum = jnp.sum(jnp.where(in_range, token_score, 0.0))
        return (layer_output, pooled_sum / length.astype(jnp.float32))
    sequences = hidden_states.reshape(SEQS, LEN, D)
    outputs, rewards = lax.map(sequence_step, (sequences, lengths))
    reward_mean = jnp.mean(rewards)
    reward_var = jnp.mean((rewards - reward_mean) * (rewards - reward_mean))
    normalized = (rewards - reward_mean) / jnp.sqrt(reward_var + 1e-06)
    return (outputs.reshape(TOKENS, D), normalized)
```

```python
import functools

import jax
import jax.numpy as jnp
from jax import lax
from jax.experimental import pallas as pl
from jax.experimental.pallas import tpu as pltpu
from jax.sharding import PartitionSpec as P

DK = 64
LEN = 512
TILE = 128

bucket_edges = (12, 16, 23, 32, 46, 64, 91)


def bucket_index(relative):
    distance = jnp.abs(relative)
    bucket_low = jnp.minimum(distance, 8)
    for threshold in bucket_edges:
        bucket_low = bucket_low + (distance >= threshold).astype(jnp.int32)
    return jnp.where(relative > 0, 16, 0) + bucket_low


def rms_norm(values_in, weight_gain):
    return (
        values_in
        * lax.rsqrt(jnp.mean(values_in * values_in, axis=-1, keepdims=True) + 1e-06)
        * weight_gain
    )


def reorder_blocks(values_in, ordering):
    full_shape = values_in.shape
    blocks = values_in.reshape(
        full_shape[:-1] + (ordering.shape[0], full_shape[-1] // ordering.shape[0])
    )
    return jnp.take(blocks, ordering, axis=-2).reshape(full_shape)


def ring_pairs(step):
    size = lax.axis_size("tensor")
    return [(i, (i + step) % size) for i in range(size)]


def ring_gather(block):
    size = lax.axis_size("tensor")
    if size != 4:
        return lax.all_gather(block, "tensor", axis=0, tiled=True)
    rows = block.shape[0]
    half = rows // 2
    here = lax.axis_index("tensor")
    before = lax.ppermute(block, "tensor", ring_pairs(1))
    after = lax.ppermute(block, "tensor", ring_pairs(-1))
    far_low = lax.ppermute(before[:half], "tensor", ring_pairs(1))
    far_high = lax.ppermute(after[half:], "tensor", ring_pairs(-1))
    whole = jnp.zeros((size * rows,) + block.shape[1:], block.dtype)
    zero = jnp.int32(0)
    for piece, shift, offset in (
        (block, 0, 0),
        (before, 3, 0),
        (after, 1, 0),
        (far_low, 2, 0),
        (far_high, 2, half),
    ):
        start = ((here + shift) % size) * rows + offset
        whole = lax.dynamic_update_slice(whole, piece, (start, zero))
    return whole


def ring_scatter(partial):
    size = lax.axis_size("tensor")
    if size != 4:
        return lax.psum_scatter(partial, "tensor", scatter_dimension=0, tiled=True).astype(
            jnp.float32
        )
    rows = partial.shape[0] // size
    half = rows // 2
    here = lax.axis_index("tensor")

    def rows_of(shift):
        start = ((here + shift) % size) * rows
        return lax.dynamic_slice(partial, (start, jnp.int32(0)), (rows, partial.shape[1]))

    far = rows_of(2)
    low = lax.ppermute(far[:half], "tensor", ring_pairs(1))
    high = lax.ppermute(far[half:], "tensor", ring_pairs(-1))
    ahead = rows_of(1)
    behind = rows_of(3)
    ahead = jnp.concatenate(
        [
            (ahead[:half].astype(jnp.float32) + low.astype(jnp.float32)).astype(partial.dtype),
            ahead[half:],
        ]
    )
    behind = jnp.concatenate(
        [
            behind[:half],
            (behind[half:].astype(jnp.float32) + high.astype(jnp.float32)).astype(partial.dtype),
        ]
    )
    from_before = lax.ppermute(ahead, "tensor", ring_pairs(1))
    from_after = lax.ppermute(behind, "tensor", ring_pairs(-1))
    return (
        rows_of(0).astype(jnp.float32)
        + from_before.astype(jnp.float32)
        + from_after.astype(jnp.float32)
    )


def attention_kernel(length_ref, q_ref, k_ref, v_ref, bias_ref, o_ref):
    span = q_ref.shape[0]
    lanes = q_ref.shape[1]
    blocks = span // TILE
    length = length_ref[0]
    keys = k_ref[...]
    values = v_ref[...]
    valid = lax.broadcasted_iota(jnp.int32, (1, span), 1) < length
    first_head = lax.broadcasted_iota(jnp.int32, (1, lanes), 1) < DK
    contexts = []
    for head in range(2):
        table = bias_ref[0, head : head + 1, :]
        near = pltpu.roll(
            jnp.broadcast_to(table, (TILE, 4 * TILE)), 0, 1, stride=1, stride_axis=0
        )
        own = first_head if head == 0 else jnp.logical_not(first_head)
        far_left = jnp.broadcast_to(table[:, 1:2], (TILE, TILE))
        far_right = jnp.broadcast_to(table[:, 4 * TILE - 1 :], (TILE, TILE))
        pieces = []
        for block in range(blocks):
            queries = q_ref[block * TILE : (block + 1) * TILE, :]
            queries = jnp.where(own, queries, jnp.zeros_like(queries))
            scores = lax.dot_general(
                queries, keys, (((1,), (1,)), ((), ())), preferred_element_type=jnp.float32
            )
            bias = []
            for other in range(blocks):
                delta = other - block
                if delta < -1:
                    bias.append(far_left)
                elif delta > 1:
                    bias.append(far_right)
                else:
                    bias.append(near[:, (delta + 2) * TILE : (delta + 3) * TILE])
            scores = jnp.where(valid, scores + jnp.concatenate(bias, axis=1), -1e30)
            top = jnp.max(scores, axis=-1, keepdims=True)
            weights = jnp.exp(scores - top)
            total = jnp.sum(weights, axis=-1, keepdims=True)
            soft = (weights / total).astype(jnp.bfloat16)
            pieces.append(jnp.dot(soft, values, preferred_element_type=jnp.float32))
        contexts.append(pieces)
    for block in range(blocks):
        o_ref[block * TILE : (block + 1) * TILE, :] = jnp.where(
            first_head, contexts[0][block], contexts[1][block]
        ).astype(o_ref.dtype)


def attention(length, projected, bias_table):
    span, width = projected.shape
    inner = width // 3
    pairs = inner // (2 * DK)
    return pl.pallas_call(
        attention_kernel,
        out_shape=jax.ShapeDtypeStruct((span, inner), jnp.bfloat16),
        grid_spec=pltpu.PrefetchScalarGridSpec(
            num_scalar_prefetch=1,
            grid=(pairs,),
            in_specs=[
                pl.BlockSpec((span, 2 * DK), lambda p, n: (0, p)),
                pl.BlockSpec((span, 2 * DK), lambda p, n: (0, pairs + p)),
                pl.BlockSpec((span, 2 * DK), lambda p, n: (0, 2 * pairs + p)),
                pl.BlockSpec((1, 2, 4 * TILE), lambda p, n: (p, 0, 0)),
            ],
            out_specs=pl.BlockSpec((span, 2 * DK), lambda p, n: (0, p)),
        ),
        cost_estimate=pl.CostEstimate(
            flops=16 * span * span * inner,
            bytes_accessed=2 * span * (width + inner),
            transcendentals=span * span * inner // DK,
        ),
        name="attention",
    )(length, projected, projected, projected, bias_table)


def total_over(values_in, name):
    size = lax.axis_size(name)
    if size > 8:
        return lax.psum(values_in, name)
    total = values_in
    for step in range(1, size):
        total = total + lax.ppermute(
            values_in, name, [(i, (i + step) % size) for i in range(size)]
        )
    return total


def local(
    hidden_states,
    lengths,
    shard_order,
    gain_attn,
    w_query,
    w_key,
    w_value,
    w_out,
    rel_bias,
    gain_ff,
    w_gate,
    w_up,
    w_down,
    gain_final,
    w_reward,
):
    groups = shard_order.shape[0]
    block_ids = jnp.arange(groups, dtype=jnp.int32)
    inverse = jnp.sum(
        block_ids[:, None] * (shard_order[:, None] == block_ids[None, :]).astype(jnp.int32), axis=0
    )
    own_rows = reorder_blocks(hidden_states, shard_order)
    attn_gain = reorder_blocks(gain_attn, shard_order)
    feed_gain = reorder_blocks(gain_ff, shard_order)
    final_gain = reorder_blocks(gain_final, shard_order)
    reward_head = reorder_blocks(w_reward, shard_order)
    row_count = own_rows.shape[0]
    row_start = lax.axis_index("tensor") * row_count

    qkv_full = lax.all_gather(
        jnp.concatenate([w_query, w_key, w_value], axis=1), "dp", axis=0, tiled=True
    )
    out_full = lax.all_gather(w_out, "dp", axis=1, tiled=True)
    gate_up_full = lax.all_gather(
        jnp.concatenate([w_gate, w_up], axis=1), "dp", axis=0, tiled=True
    )
    down_full = lax.all_gather(w_down, "dp", axis=1, tiled=True)

    normed = ring_gather(rms_norm(own_rows, attn_gain).astype(jnp.bfloat16))
    projected = jnp.dot(normed, qkv_full, preferred_element_type=jnp.float32).astype(jnp.bfloat16)

    heads = rel_bias.shape[1]
    relative = jnp.arange(4 * TILE, dtype=jnp.int32) - 2 * TILE
    onehot = (
        bucket_index(relative)[:, None]
        == jnp.arange(rel_bias.shape[0], dtype=jnp.int32)[None, :]
    ).astype(jnp.float32)
    bias_table = jnp.dot(onehot, rel_bias, precision=lax.Precision.HIGHEST).T
    bias_table = bias_table.reshape(heads // 2, 2, 4 * TILE)
    length = lengths[0]
    context = attention(lengths, projected, bias_table)

    attn_partial = jnp.dot(context, out_full, preferred_element_type=jnp.float32).astype(
        jnp.bfloat16
    )
    mid_own = own_rows + ring_scatter(attn_partial)
    mid_normed = ring_gather(rms_norm(mid_own, feed_gain).astype(jnp.bfloat16))
    hidden_width = w_gate.shape[1]
    gate_up = jnp.dot(mid_normed, gate_up_full, preferred_element_type=jnp.float32)
    activated = (
        jax.nn.gelu(gate_up[:, :hidden_width], approximate=True) * gate_up[:, hidden_width:]
    ).astype(jnp.bfloat16)
    feed_partial = jnp.dot(activated, down_full, preferred_element_type=jnp.float32).astype(
        jnp.bfloat16
    )
    output_rows = mid_own + ring_scatter(feed_partial)
    final_normed = rms_norm(output_rows, final_gain)
    token_score = jnp.dot(final_normed, reward_head, precision=lax.Precision.HIGHEST)
    positions = row_start + jnp.arange(row_count, dtype=jnp.int32)
    local_pool = jnp.sum(jnp.where(positions < length, token_score, 0.0))
    pooled_sum = total_over(jnp.reshape(local_pool, (1,)), "tensor")
    reward = pooled_sum / length.astype(jnp.float32)
    rollouts = lax.axis_size("dp") * lengths.shape[0]
    moments = total_over(jnp.concatenate([reward, reward * reward]), "dp")
    reward_mean = moments[0] / rollouts
    reward_var = moments[1] / rollouts - reward_mean * reward_mean
    normalized = (reward - reward_mean) / jnp.sqrt(reward_var + 1e-06)
    return (reorder_blocks(output_rows, inverse), normalized)


def solution(mesh):
    placed = (
        P(("dp", "tensor"), None),
        P("dp"),
        P(),
        P(),
        P("dp", "tensor"),
        P("dp", "tensor"),
        P("dp", "tensor"),
        P("tensor", "dp"),
        P(None, "tensor"),
        P(),
        P("dp", "tensor"),
        P("dp", "tensor"),
        P("tensor", "dp"),
        P(),
        P(),
    )
    return jax.shard_map(
        local,
        mesh=mesh,
        in_specs=placed,
        out_specs=(P(("dp", "tensor"), None), P("dp")),
        check_vma=False,
    )
```

```python
import functools

import jax
import jax.numpy as jnp
from jax import lax
from jax.experimental import pallas as pl
from jax.experimental.pallas import tpu as pltpu
from jax.sharding import PartitionSpec as P


DK = 64
TILE = 128

bucket_edges = (12, 16, 23, 32, 46, 64, 91)


def bucket_index(relative):
    distance = jnp.abs(relative)
    bucket_low = jnp.minimum(distance, 8)
    for threshold in bucket_edges:
        bucket_low = bucket_low + (distance >= threshold).astype(jnp.int32)
    return jnp.where(relative > 0, 16, 0) + bucket_low


def rms_norm(values_in, weight_gain):
    return (
        values_in
        * lax.rsqrt(jnp.mean(values_in * values_in, axis=-1, keepdims=True) + 1e-06)
        * weight_gain
    )


def reorder_blocks(values_in, ordering):
    full_shape = values_in.shape
    blocks = values_in.reshape(
        full_shape[:-1] + (ordering.shape[0], full_shape[-1] // ordering.shape[0])
    )
    return jnp.take(blocks, ordering, axis=-2).reshape(full_shape)


def ring_pairs(step):
    size = lax.axis_size("tensor")
    return [(i, (i + step) % size) for i in range(size)]


def ring_gather(block):
    size = lax.axis_size("tensor")
    if size != 4:
        return lax.all_gather(block, "tensor", axis=0, tiled=True)
    rows = block.shape[0]
    half = rows // 2
    here = lax.axis_index("tensor")
    before = lax.ppermute(block, "tensor", ring_pairs(1))
    after = lax.ppermute(block, "tensor", ring_pairs(-1))
    far_low = lax.ppermute(before[:half], "tensor", ring_pairs(1))
    far_high = lax.ppermute(after[half:], "tensor", ring_pairs(-1))
    whole = jnp.zeros((size * rows,) + block.shape[1:], block.dtype)
    zero = jnp.int32(0)
    for piece, shift, offset in (
        (block, 0, 0),
        (before, 3, 0),
        (after, 1, 0),
        (far_low, 2, 0),
        (far_high, 2, half),
    ):
        start = ((here + shift) % size) * rows + offset
        whole = lax.dynamic_update_slice(whole, piece, (start, zero))
    return whole


def ring_scatter(partial):
    size = lax.axis_size("tensor")
    if size != 4:
        return lax.psum_scatter(partial, "tensor", scatter_dimension=0, tiled=True).astype(
            jnp.float32
        )
    rows = partial.shape[0] // size
    half = rows // 2
    here = lax.axis_index("tensor")

    def rows_of(shift):
        start = ((here + shift) % size) * rows
        return lax.dynamic_slice(partial, (start, jnp.int32(0)), (rows, partial.shape[1]))

    far = rows_of(2)
    low = lax.ppermute(far[:half], "tensor", ring_pairs(1))
    high = lax.ppermute(far[half:], "tensor", ring_pairs(-1))
    ahead = rows_of(1)
    behind = rows_of(3)
    ahead = jnp.concatenate(
        [
            (ahead[:half].astype(jnp.float32) + low.astype(jnp.float32)).astype(partial.dtype),
            ahead[half:],
        ]
    )
    behind = jnp.concatenate(
        [
            behind[:half],
            (behind[half:].astype(jnp.float32) + high.astype(jnp.float32)).astype(partial.dtype),
        ]
    )
    from_before = lax.ppermute(ahead, "tensor", ring_pairs(1))
    from_after = lax.ppermute(behind, "tensor", ring_pairs(-1))
    return (
        rows_of(0).astype(jnp.float32)
        + from_before.astype(jnp.float32)
        + from_after.astype(jnp.float32)
    )


def attention_kernel(length_ref, q_ref, k_ref, v_ref, bias_ref, o_ref):
    span = q_ref.shape[0]
    lanes = q_ref.shape[1]
    blocks = span // TILE
    length = length_ref[0]
    keys = k_ref[...]
    values = v_ref[...]
    valid = lax.broadcasted_iota(jnp.int32, (1, span), 1) < length
    first_head = lax.broadcasted_iota(jnp.int32, (1, lanes), 1) < DK
    contexts = []
    for head in range(2):
        table = bias_ref[0, head : head + 1, :]
        near = pltpu.roll(
            jnp.broadcast_to(table, (TILE, 4 * TILE)), 0, 1, stride=1, stride_axis=0
        )
        own = first_head if head == 0 else jnp.logical_not(first_head)
        far_left = jnp.broadcast_to(table[:, 1:2], (TILE, TILE))
        far_right = jnp.broadcast_to(table[:, 4 * TILE - 1 :], (TILE, TILE))
        pieces = []
        for block in range(blocks):
            queries = q_ref[block * TILE : (block + 1) * TILE, :]
            queries = jnp.where(own, queries, jnp.zeros_like(queries))
            scores = lax.dot_general(
                queries, keys, (((1,), (1,)), ((), ())), preferred_element_type=jnp.float32
            )
            bias = []
            for other in range(blocks):
                delta = other - block
                if delta < -1:
                    bias.append(far_left)
                elif delta > 1:
                    bias.append(far_right)
                else:
                    bias.append(near[:, (delta + 2) * TILE : (delta + 3) * TILE])
            scores = jnp.where(valid, scores + jnp.concatenate(bias, axis=1), -1e30)
            top = jnp.max(scores, axis=-1, keepdims=True)
            weights = jnp.exp(scores - top)
            total = jnp.sum(weights, axis=-1, keepdims=True)
            soft = (weights / total).astype(jnp.bfloat16)
            pieces.append(jnp.dot(soft, values, preferred_element_type=jnp.float32))
        contexts.append(pieces)
    for block in range(blocks):
        o_ref[block * TILE : (block + 1) * TILE, :] = jnp.where(
            first_head, contexts[0][block], contexts[1][block]
        ).astype(o_ref.dtype)


def attention(length, projected, bias_table):
    span, width = projected.shape
    inner = width // 3
    pairs = inner // (2 * DK)
    return pl.pallas_call(
        attention_kernel,
        out_shape=jax.ShapeDtypeStruct((span, inner), jnp.bfloat16),
        grid_spec=pltpu.PrefetchScalarGridSpec(
            num_scalar_prefetch=1,
            grid=(pairs,),
            in_specs=[
                pl.BlockSpec((span, 2 * DK), lambda p, n: (0, p)),
                pl.BlockSpec((span, 2 * DK), lambda p, n: (0, pairs + p)),
                pl.BlockSpec((span, 2 * DK), lambda p, n: (0, 2 * pairs + p)),
                pl.BlockSpec((1, 2, 4 * TILE), lambda p, n: (p, 0, 0)),
            ],
            out_specs=pl.BlockSpec((span, 2 * DK), lambda p, n: (0, p)),
        ),
        cost_estimate=pl.CostEstimate(
            flops=16 * span * span * inner,
            bytes_accessed=2 * span * (width + inner),
            transcendentals=span * span * inner // DK,
        ),
        name="attention",
    )(length, projected, projected, projected, bias_table)


def total_over(values_in, name):
    size = lax.axis_size(name)
    if size > 8:
        return lax.psum(values_in, name)
    total = values_in
    for step in range(1, size):
        total = total + lax.ppermute(
            values_in, name, [(i, (i + step) % size) for i in range(size)]
        )
    return total


def local_general(
    hidden_states,
    lengths,
    shard_order,
    gain_attn,
    w_query,
    w_key,
    w_value,
    w_out,
    rel_bias,
    gain_ff,
    w_gate,
    w_up,
    w_down,
    gain_final,
    w_reward,
):
    groups = shard_order.shape[0]
    block_ids = jnp.arange(groups, dtype=jnp.int32)
    inverse = jnp.sum(
        block_ids[:, None] * (shard_order[:, None] == block_ids[None, :]).astype(jnp.int32), axis=0
    )
    own_rows = reorder_blocks(hidden_states, shard_order)
    attn_gain = reorder_blocks(gain_attn, shard_order)
    feed_gain = reorder_blocks(gain_ff, shard_order)
    final_gain = reorder_blocks(gain_final, shard_order)
    reward_head = reorder_blocks(w_reward, shard_order)
    row_count = own_rows.shape[0]
    row_start = lax.axis_index("tensor") * row_count

    qkv_full = lax.all_gather(
        jnp.concatenate([w_query, w_key, w_value], axis=1), "dp", axis=0, tiled=True
    )
    out_full = lax.all_gather(w_out, "dp", axis=1, tiled=True)
    gate_up_full = lax.all_gather(
        jnp.concatenate([w_gate, w_up], axis=1), "dp", axis=0, tiled=True
    )
    down_full = lax.all_gather(w_down, "dp", axis=1, tiled=True)

    normed = ring_gather(rms_norm(own_rows, attn_gain).astype(jnp.bfloat16))
    projected = jnp.dot(normed, qkv_full, preferred_element_type=jnp.float32).astype(jnp.bfloat16)

    heads = rel_bias.shape[1]
    relative = jnp.arange(4 * TILE, dtype=jnp.int32) - 2 * TILE
    onehot = (
        bucket_index(relative)[:, None]
        == jnp.arange(rel_bias.shape[0], dtype=jnp.int32)[None, :]
    ).astype(jnp.float32)
    bias_table = jnp.dot(onehot, rel_bias, precision=lax.Precision.HIGHEST).T
    bias_table = bias_table.reshape(heads // 2, 2, 4 * TILE)
    length = lengths[0]
    context = attention(lengths, projected, bias_table)

    attn_partial = jnp.dot(context, out_full, preferred_element_type=jnp.float32).astype(
        jnp.bfloat16
    )
    mid_own = own_rows + ring_scatter(attn_partial)
    mid_normed = ring_gather(rms_norm(mid_own, feed_gain).astype(jnp.bfloat16))
    hidden_width = w_gate.shape[1]
    gate_up = jnp.dot(mid_normed, gate_up_full, preferred_element_type=jnp.float32)
    activated = (
        jax.nn.gelu(gate_up[:, :hidden_width], approximate=True) * gate_up[:, hidden_width:]
    ).astype(jnp.bfloat16)
    feed_partial = jnp.dot(activated, down_full, preferred_element_type=jnp.float32).astype(
        jnp.bfloat16
    )
    output_rows = mid_own + ring_scatter(feed_partial)
    final_normed = rms_norm(output_rows, final_gain)
    token_score = jnp.dot(final_normed, reward_head, precision=lax.Precision.HIGHEST)
    positions = row_start + jnp.arange(row_count, dtype=jnp.int32)
    local_pool = jnp.sum(jnp.where(positions < length, token_score, 0.0))
    pooled_sum = total_over(jnp.reshape(local_pool, (1,)), "tensor")
    reward = pooled_sum / length.astype(jnp.float32)
    rollouts = lax.axis_size("dp") * lengths.shape[0]
    moments = total_over(jnp.concatenate([reward, reward * reward]), "dp")
    reward_mean = moments[0] / rollouts
    reward_var = moments[1] / rollouts - reward_mean * reward_mean
    normalized = (reward - reward_mean) / jnp.sqrt(reward_var + 1e-06)
    return (reorder_blocks(output_rows, inverse), normalized)


def put(ref, rows, value):
    ref[pl.ds(pl.multiple_of(rows, TILE // 2), value.shape[0]), :] = value


def slot_row(ids, shift, rows):
    return lax.rem(ids[1] + shift, 4) * rows


def true_block(order, ids, mask):
    return order[lax.bitwise_xor(ids[0], jnp.int32(mask))]


PARTS = ((0, 0), (1, 0), (2, 0), (3, 0), (4, 0), (5, 0), (6, 0), (6, 1), (7, 0), (7, 1))


def placed_rows(order, ids, blocks, block):
    for ref, (mask, part) in zip(blocks, PARTS):
        start = true_block(order, ids, mask) * block + part * (block // 2)
        yield ref, pl.multiple_of(start, block // 2)


def rms_kernel(x_ref, gain_ref, low_ref, high_ref):
    x = x_ref[...]
    scale = lax.rsqrt(jnp.mean(x * x, axis=-1, keepdims=True) + 1e-06)
    normed = (x * scale * gain_ref[...]).astype(jnp.bfloat16)
    half = low_ref.shape[0]
    low_ref[...] = normed[:half]
    high_ref[...] = normed[half:]


def pack_kernel(*refs):
    *sources, out = refs
    rows, at = out.shape[0], 0
    step = 2 * TILE
    wide = [s for s in sources if s.shape[0] == rows]
    tall = [s for s in sources if s.shape[0] != rows]
    if tall:
        for j in range(wide[0].shape[1] // step):
            for s in wide:
                out[:, at : at + step] = s[:, j * step : (j + 1) * step]
                at += step
        for s in tall:
            for j in range(s.shape[0] // rows):
                out[:, at : at + s.shape[1]] = s[j * rows : (j + 1) * rows, :]
                at += s.shape[1]
    else:
        for s in wide:
            out[:, at : at + s.shape[1]] = s[...]
            at += s.shape[1]


def project_kernel(order, ids, *refs):
    pieces = refs[:8]
    blocks = refs[8:18]
    out, x_all, w_all, sems = refs[18:]
    tiles, depth, wide = w_all.shape
    for j in range(tiles):
        for ref, start in placed_rows(order, ids, blocks, depth // 8):
            pltpu.make_async_copy(
                ref.at[:, pl.ds(j * wide, wide)],
                w_all.at[j, pl.ds(start, ref.shape[0]), :],
                sems.at[j],
            ).start()
    rows = pieces[0].shape[0]
    for slot, shift in enumerate((0, 3, 1, 2)):
        base = slot_row(ids, shift, 2 * rows)
        put(x_all, base, pieces[2 * slot][...])
        put(x_all, base + rows, pieces[2 * slot + 1][...])

    @pl.loop(0, tiles)
    def _(j):
        pltpu.make_async_copy(w_all.at[j], w_all.at[j], sems.at[j]).wait()
        out[:, pl.ds(pl.multiple_of(j * wide, wide), wide)] = jnp.dot(
            x_all[...], w_all[j], preferred_element_type=jnp.float32
        ).astype(out.dtype)


def out_kernel(order, ids, context, *refs):
    blocks = refs[:8]
    far_low, far_high, ahead_low, ahead_high, behind_low, behind_high, own = refs[8:15]
    x_all, w_all, sems = refs[15:]
    for mask in range(8):
        where_to = true_block(order, ids, mask)
        pltpu.make_async_copy(blocks[mask], w_all.at[where_to], sems.at[where_to]).start()
    rows = own.shape[0]
    half = rows // 2
    for slot, shift in enumerate((2, 1, 3, 0)):
        start = pl.multiple_of(slot_row(ids, shift, rows), rows)
        x_all[slot * rows : (slot + 1) * rows, :] = context[pl.ds(start, rows), :]
    wide = w_all.shape[2]

    @pl.loop(0, 8)
    def _(n):
        pltpu.make_async_copy(w_all.at[n], w_all.at[n], sems.at[n]).wait()
        columns = pl.ds(pl.multiple_of(n * wide, wide), wide)
        part = jnp.dot(x_all[...], w_all[n], preferred_element_type=jnp.float32).astype(own.dtype)
        for k, ref in enumerate(
            (far_low, far_high, ahead_low, ahead_high, behind_low, behind_high)
        ):
            ref[:, columns] = part[k * half : (k + 1) * half, :]
        own[:, columns] = part[3 * rows :, :]


def gelu(v):
    return 0.5 * v * (1.0 + jnp.tanh(0.7978845608028654 * (v + 0.044715 * (v * v * v))))


def feed_kernel(count, order, ids, *refs):
    pieces = refs[:count]
    blocks = refs[count : count + 10]
    outs = refs[count + 10 : 2 * count + 10]
    x_all, hidden, first, second, sem_first, sem_second = refs[2 * count + 10 :]
    tiles, depth, wide = first.shape
    block = depth // 8
    unit = wide // 2
    for j in range(tiles):
        for ref, start in placed_rows(order, ids, blocks, block):
            pltpu.make_async_copy(
                ref.at[:, pl.ds(j * wide, wide)],
                first.at[j, pl.ds(start, ref.shape[0]), :],
                sem_first.at[j],
            ).start()
    for ref, (mask, part) in zip(blocks, PARTS):
        where_to = true_block(order, ids, mask)
        for j in range(second.shape[1] // block):
            pltpu.make_async_copy(
                ref.at[:, pl.ds(tiles * wide + j * block, block)],
                second.at[
                    where_to, pl.ds(j * block + part * (block // 2), ref.shape[0]), :
                ],
                sem_second.at[where_to],
            ).start()
    rows = pieces[0].shape[0]
    for k in range(count):
        x_all[k * rows : (k + 1) * rows, :] = pieces[k][...]

    @pl.loop(0, tiles)
    def _(j):
        pltpu.make_async_copy(first.at[j], first.at[j], sem_first.at[j]).wait()
        both = jnp.dot(x_all[...], first[j], preferred_element_type=jnp.float32)
        hidden[:, pl.ds(pl.multiple_of(j * unit, unit), unit)] = (
            gelu(both[:, :unit]) * both[:, unit:]
        ).astype(hidden.dtype)

    @pl.loop(0, 8)
    def _(n):
        pltpu.make_async_copy(second.at[n], second.at[n], sem_second.at[n]).wait()
        columns = pl.ds(pl.multiple_of(n * block, block), block)
        part = jnp.dot(hidden[...], second[n], preferred_element_type=jnp.float32).astype(
            outs[0].dtype
        )
        for k in range(count):
            outs[k][:, columns] = part[k * rows : (k + 1) * rows, :]


def residual(base, shares, half):
    own, before_low, before_high, after_low, after_high = shares
    low = base[:half] + (
        own[:half].astype(jnp.float32)
        + before_low[...].astype(jnp.float32)
        + after_low[...].astype(jnp.float32)
    )
    high = base[half:] + (
        own[half:].astype(jnp.float32)
        + before_high[...].astype(jnp.float32)
        + after_high[...].astype(jnp.float32)
    )
    return low, high


def mid_kernel(x_ref, *refs):
    shares, gain_ref, mid_ref, low_ref, high_ref = refs[:5], *refs[5:]
    half = low_ref.shape[0]
    for k, part in enumerate(residual(x_ref, shares, half)):
        mid_ref[k * half : (k + 1) * half, :] = part
        scale = lax.rsqrt(jnp.mean(part * part, axis=-1, keepdims=True) + 1e-06)
        (low_ref, high_ref)[k][...] = (part * scale * gain_ref[...]).astype(jnp.bfloat16)


def final_kernel(length, ids, x_ref, *refs):
    shares, gain_ref, head_ref, out_ref, pool_ref = refs[:5], *refs[5:]
    half = out_ref.shape[0] // 2
    pooled = jnp.zeros((1, 1), jnp.float32)
    for k, part in enumerate(residual(x_ref, shares, half)):
        out_ref[k * half : (k + 1) * half, :] = part
        scale = lax.rsqrt(jnp.mean(part * part, axis=-1, keepdims=True) + 1e-06)
        score = jnp.sum(part * scale * gain_ref[...] * head_ref[...], axis=-1, keepdims=True)
        position = (
            lax.broadcasted_iota(jnp.int32, (half, 1), 0) + ids[1] * (2 * half) + k * half
        )
        pooled = pooled + jnp.sum(
            jnp.where(position < length[0], score, 0.0), axis=0, keepdims=True
        )
    pool_ref[...] = jnp.broadcast_to(pooled, pool_ref.shape)


def whole(array):
    return pl.BlockSpec(array.shape, lambda *_: (0,) * len(array.shape))


def call(kernel, scalars, arrays, raw, outs, scratch, flops, moved):
    single = not isinstance(outs, (list, tuple))
    out_list = [outs] if single else list(outs)
    result = pl.pallas_call(
      kernel,
      out_shape=out_list,
      grid_spec=pltpu.PrefetchScalarGridSpec(
          num_scalar_prefetch=len(scalars),
          grid=(1,),
          in_specs=[whole(a) for a in arrays]
          + [pl.BlockSpec(memory_space=pl.ANY) for _ in raw],
          out_specs=[whole(o) for o in out_list],
          scratch_shapes=scratch,
      ),
      cost_estimate=pl.CostEstimate(flops=flops, bytes_accessed=moved, transcendentals=0),
    )(*scalars, *arrays, *raw)
    return result[0] if single else result


def shift_rows(block, step):
    return lax.ppermute(block, "tensor", ring_pairs(step))


def exchange(block, mask):
    return lax.ppermute(block, "dp", [(i, i ^ mask) for i in range(8)])


def plane_gather(block):
    held = {0: block}
    for mask in (2, 4, 6, 1):
        held[mask] = exchange(block, mask)
    for mask in (3, 5, 7):
        held[mask] = exchange(held[mask ^ 1], 1)
    return [held[mask] for mask in range(8)]


def plane_gather_split(block):
    half = block.shape[0] // 2
    held = {0: block}
    for mask in (2, 4, 1):
        held[mask] = exchange(block, mask)
    low = exchange(held[4][:half], 2)
    high = exchange(held[2][half:], 4)
    for mask in (3, 5):
        held[mask] = exchange(held[mask ^ 1], 1)
    pairs = [exchange(low, 1), exchange(high, 1)]
    return [held[mask] for mask in range(6)] + [low, high] + pairs


def half_gather(low, high):
    before_low = shift_rows(low, 1)
    after_high = shift_rows(high, -1)
    before_high = shift_rows(high, 1)
    after_low = shift_rows(low, -1)
    far_low = shift_rows(before_low, 1)
    far_high = shift_rows(after_high, -1)
    return [low, high, before_low, before_high, after_low, after_high, far_low, far_high]


def add_share(mine, received):
    return (mine.astype(jnp.float32) + received.astype(jnp.float32)).astype(mine.dtype)


def half_scatter(far_low, far_high, ahead_low, ahead_high, behind_low, behind_high, own):
    low = shift_rows(far_low, 1)
    high = shift_rows(far_high, -1)
    before_high = shift_rows(ahead_high, 1)
    after_low = shift_rows(behind_low, -1)
    before_low = shift_rows(add_share(ahead_low, low), 1)
    after_high = shift_rows(add_share(behind_high, high), -1)
    return [own, before_low, before_high, after_low, after_high]


def layer(
    hidden_states,
    lengths,
    shard_order,
    gain_attn,
    w_query,
    w_key,
    w_value,
    w_out,
    rel_bias,
    gain_ff,
    w_gate,
    w_up,
    w_down,
    gain_final,
    w_reward,
):
    bf16, f32 = jnp.bfloat16, jnp.float32
    shape = jax.ShapeDtypeStruct
    rows, width = hidden_states.shape
    half = rows // 2
    length_all = 4 * rows
    block = w_query.shape[0]
    inner = w_query.shape[1]
    hidden = w_gate.shape[1]
    ids = jnp.stack([lax.axis_index("dp"), lax.axis_index("tensor")]).astype(jnp.int32)
    half_bf = shape((half, width), bf16)
    row_bf = shape((rows, width), bf16)
    row_f32 = shape((rows, width), f32)

    qkv_own = call(
        pack_kernel, [], [w_query, w_key, w_value], [],
        shape((block, 3 * inner), bf16), [], 2 * block * inner, 12 * block * inner,
    )
    low, high = call(
        rms_kernel, [], [hidden_states, gain_attn.reshape(1, width)], [],
        [half_bf, half_bf], [], 4 * rows * width, 6 * rows * width,
    )
    normed = half_gather(low, high)
    qkv = plane_gather_split(qkv_own)
    out_blocks = plane_gather(w_out)
    feed_own = call(
        pack_kernel, [], [w_gate, w_up, w_down], [],
        shape((block, 3 * hidden), bf16), [], 2 * block * hidden, 12 * block * hidden,
    )
    feed = plane_gather_split(feed_own)

    tile = 2 * TILE
    projected = call(
        project_kernel, [shard_order, ids], normed, qkv,
        shape((length_all, 3 * inner), bf16),
        [
            pltpu.VMEM((length_all, width), bf16),
            pltpu.VMEM((3 * inner // tile, width, tile), bf16),
            pltpu.SemaphoreType.DMA((3 * inner // tile,)),
        ],
        6 * length_all * width * inner, 6 * width * inner,
    )

    heads = rel_bias.shape[1]
    relative = jnp.arange(4 * TILE, dtype=jnp.int32) - 2 * TILE
    onehot = (
        bucket_index(relative)[:, None]
        == jnp.arange(rel_bias.shape[0], dtype=jnp.int32)[None, :]
    ).astype(f32)
    bias_table = jnp.dot(onehot, rel_bias, precision=lax.Precision.HIGHEST).T
    context = attention(lengths, projected, bias_table.reshape(heads // 2, 2, 4 * TILE))

    parts = call(
        out_kernel, [shard_order, ids], [context], out_blocks,
        [half_bf] * 6 + [row_bf],
        [
            pltpu.VMEM((length_all, inner), bf16),
            pltpu.VMEM((8, inner, block), bf16),
            pltpu.SemaphoreType.DMA((8,)),
        ],
        2 * length_all * width * inner, 2 * width * inner,
    )
    mid, low, high = call(
        mid_kernel, [],
        [hidden_states, *half_scatter(*parts), gain_ff.reshape(1, width)], [],
        [row_f32, half_bf, half_bf], [], 8 * rows * width, 16 * rows * width,
    )
    normed = half_gather(low, high)

    def feed_forward(pieces):
        count = len(pieces)
        return call(
            functools.partial(feed_kernel, count), [shard_order, ids], pieces, feed,
            [half_bf] * count,
            [
                pltpu.VMEM((count * half, width), bf16),
                pltpu.VMEM((count * half, hidden), bf16),
                pltpu.VMEM((hidden // tile, width, 2 * tile), bf16),
                pltpu.VMEM((8, hidden, block), bf16),
                pltpu.SemaphoreType.DMA((hidden // tile,)),
                pltpu.SemaphoreType.DMA((8,)),
            ],
            6 * count * half * width * hidden, 6 * width * hidden,
        )

    near = feed_forward(normed[:6])
    far = feed_forward(normed[6:])
    own = jnp.concatenate(near[:2])
    shares = half_scatter(far[0], far[1], near[4], near[5], near[2], near[3], own)
    output_rows, pool = call(
        final_kernel, [lengths, ids],
        [mid, *shares, gain_final.reshape(1, width), w_reward.reshape(1, width)], [],
        [row_f32, shape((8, TILE), f32)], [], 8 * rows * width, 16 * rows * width,
    )
    total = pool
    for step in (1, 2):
        total = total + lax.ppermute(total, "tensor", [(i, i ^ step) for i in range(4)])
    reward = total / lengths[0].astype(f32)
    moments = jnp.where(lax.broadcasted_iota(jnp.int32, reward.shape, 0) == 0, reward, reward * reward)
    for mask in (1, 2, 4):
        moments = moments + exchange(moments, mask)
    reward_mean = moments[0, 0] / 8
    reward_var = moments[1, 0] / 8 - reward_mean * reward_mean
    normalized = (reward[0, 0] - reward_mean) / jnp.sqrt(reward_var + 1e-06)
    return (output_rows, jnp.reshape(normalized, (1,)))


def local_fast(*args):
    return layer(*args)


def solution(mesh):
    placed = (
        P(("dp", "tensor"), None),
        P("dp"),
        P(),
        P(),
        P("dp", "tensor"),
        P("dp", "tensor"),
        P("dp", "tensor"),
        P("tensor", "dp"),
        P(None, "tensor"),
        P(),
        P("dp", "tensor"),
        P("dp", "tensor"),
        P("tensor", "dp"),
        P(),
        P(),
    )
    fits = mesh.shape["dp"] == 8 and mesh.shape["tensor"] == 4
    return jax.shard_map(
        local_fast if fits else local_general,
        mesh=mesh,
        in_specs=placed,
        out_specs=(P(("dp", "tensor"), None), P("dp")),
        check_vma=False,
    )
```

```python
import functools

import jax
import jax.numpy as jnp
from jax import lax
from jax.experimental import pallas as pl
from jax.experimental.pallas import tpu as pltpu
from jax.sharding import PartitionSpec as P


DK = 64
TILE = 128

bucket_edges = (12, 16, 23, 32, 46, 64, 91)


def bucket_index(relative):
    distance = jnp.abs(relative)
    bucket_low = jnp.minimum(distance, 8)
    for threshold in bucket_edges:
        bucket_low = bucket_low + (distance >= threshold).astype(jnp.int32)
    return jnp.where(relative > 0, 16, 0) + bucket_low


def rms_norm(values_in, weight_gain):
    return (
        values_in
        * lax.rsqrt(jnp.mean(values_in * values_in, axis=-1, keepdims=True) + 1e-06)
        * weight_gain
    )


def reorder_blocks(values_in, ordering):
    full_shape = values_in.shape
    blocks = values_in.reshape(
        full_shape[:-1] + (ordering.shape[0], full_shape[-1] // ordering.shape[0])
    )
    return jnp.take(blocks, ordering, axis=-2).reshape(full_shape)


def ring_pairs(step):
    size = lax.axis_size("tensor")
    return [(i, (i + step) % size) for i in range(size)]


def ring_gather(block):
    size = lax.axis_size("tensor")
    if size != 4:
        return lax.all_gather(block, "tensor", axis=0, tiled=True)
    rows = block.shape[0]
    half = rows // 2
    here = lax.axis_index("tensor")
    before = lax.ppermute(block, "tensor", ring_pairs(1))
    after = lax.ppermute(block, "tensor", ring_pairs(-1))
    far_low = lax.ppermute(before[:half], "tensor", ring_pairs(1))
    far_high = lax.ppermute(after[half:], "tensor", ring_pairs(-1))
    whole = jnp.zeros((size * rows,) + block.shape[1:], block.dtype)
    zero = jnp.int32(0)
    for piece, shift, offset in (
        (block, 0, 0),
        (before, 3, 0),
        (after, 1, 0),
        (far_low, 2, 0),
        (far_high, 2, half),
    ):
        start = ((here + shift) % size) * rows + offset
        whole = lax.dynamic_update_slice(whole, piece, (start, zero))
    return whole


def ring_scatter(partial):
    size = lax.axis_size("tensor")
    if size != 4:
        return lax.psum_scatter(partial, "tensor", scatter_dimension=0, tiled=True).astype(
            jnp.float32
        )
    rows = partial.shape[0] // size
    half = rows // 2
    here = lax.axis_index("tensor")

    def rows_of(shift):
        start = ((here + shift) % size) * rows
        return lax.dynamic_slice(partial, (start, jnp.int32(0)), (rows, partial.shape[1]))

    far = rows_of(2)
    low = lax.ppermute(far[:half], "tensor", ring_pairs(1))
    high = lax.ppermute(far[half:], "tensor", ring_pairs(-1))
    ahead = rows_of(1)
    behind = rows_of(3)
    ahead = jnp.concatenate(
        [
            (ahead[:half].astype(jnp.float32) + low.astype(jnp.float32)).astype(partial.dtype),
            ahead[half:],
        ]
    )
    behind = jnp.concatenate(
        [
            behind[:half],
            (behind[half:].astype(jnp.float32) + high.astype(jnp.float32)).astype(partial.dtype),
        ]
    )
    from_before = lax.ppermute(ahead, "tensor", ring_pairs(1))
    from_after = lax.ppermute(behind, "tensor", ring_pairs(-1))
    return (
        rows_of(0).astype(jnp.float32)
        + from_before.astype(jnp.float32)
        + from_after.astype(jnp.float32)
    )


def attention_kernel(length_ref, q_ref, k_ref, v_ref, bias_ref, o_ref):
    span, lanes = q_ref.shape
    blocks = span // TILE
    length = length_ref[0]
    keys = k_ref[...]
    values = v_ref[...]
    masked = jnp.where(lax.broadcasted_iota(jnp.int32, (1, span), 1) < length, 0.0, -1e30)
    first = lax.broadcasted_iota(jnp.int32, (1, lanes), 1) < DK
    one = jnp.ones_like(values)
    sums = []
    for head in range(2):
        table = bias_ref[0, head : head + 1, :]
        near = pltpu.roll(jnp.broadcast_to(table, (TILE, 4 * TILE)), 0, 1, stride=1, stride_axis=0)
        own = first if head == 0 else jnp.logical_not(first)
        with_ones = jnp.where(own, values, one)
        far_left, far_right = table[:, 1:2], table[:, 4 * TILE - 1 :]
        heads = []
        for block in range(blocks):
            queries = q_ref[block * TILE : (block + 1) * TILE, :]
            queries = jnp.where(own, queries, jnp.zeros_like(queries))
            scores = lax.dot_general(queries, keys, (((1,), (1,)), ((), ())), preferred_element_type=jnp.float32)
            pieces = []
            for other in range(blocks):
                at = slice(other * TILE, (other + 1) * TILE)
                delta = other - block
                if abs(delta) > 1:
                    bias = masked[:, at] + (far_left if delta < 0 else far_right)
                    pieces.append(scores[:, at] + bias)
                else:
                    pieces.append(scores[:, at] + near[:, (delta + 2) * TILE : (delta + 3) * TILE] + masked[:, at])
            top = jnp.max(functools.reduce(jnp.maximum, pieces), axis=-1, keepdims=True)
            soft = jnp.concatenate([jnp.exp(p - top).astype(jnp.bfloat16) for p in pieces], axis=1)
            heads.append(jnp.dot(soft, with_ones, preferred_element_type=jnp.float32))
        sums.append(heads)
    for block in range(blocks):
        zero, last = sums[0][block], sums[1][block]
        total = pltpu.roll(jnp.where(first, last, zero), DK, 1)
        o_ref[block * TILE : (block + 1) * TILE, :] = (jnp.where(first, zero, last) / total).astype(o_ref.dtype)


def attention(length, projected, bias_table):
    span, width = projected.shape
    inner = width // 3
    pairs = inner // (2 * DK)
    return pl.pallas_call(
        attention_kernel,
        out_shape=jax.ShapeDtypeStruct((span, inner), jnp.bfloat16),
        grid_spec=pltpu.PrefetchScalarGridSpec(
            num_scalar_prefetch=1,
            grid=(pairs,),
            in_specs=[
                pl.BlockSpec((span, 2 * DK), lambda p, n: (0, p)),
                pl.BlockSpec((span, 2 * DK), lambda p, n: (0, pairs + p)),
                pl.BlockSpec((span, 2 * DK), lambda p, n: (0, 2 * pairs + p)),
                pl.BlockSpec((1, 2, 4 * TILE), lambda p, n: (p, 0, 0)),
            ],
            out_specs=pl.BlockSpec((span, 2 * DK), lambda p, n: (0, p)),
        ),
        cost_estimate=pl.CostEstimate(
            flops=16 * span * span * inner,
            bytes_accessed=2 * span * (width + inner),
            transcendentals=span * span * inner // DK,
        ),
        name="attention",
    )(length, projected, projected, projected, bias_table)


def total_over(values_in, name):
    size = lax.axis_size(name)
    if size > 8:
        return lax.psum(values_in, name)
    total = values_in
    for step in range(1, size):
        total = total + lax.ppermute(
            values_in, name, [(i, (i + step) % size) for i in range(size)]
        )
    return total


def local_general(
    hidden_states,
    lengths,
    shard_order,
    gain_attn,
    w_query,
    w_key,
    w_value,
    w_out,
    rel_bias,
    gain_ff,
    w_gate,
    w_up,
    w_down,
    gain_final,
    w_reward,
):
    groups = shard_order.shape[0]
    block_ids = jnp.arange(groups, dtype=jnp.int32)
    inverse = jnp.sum(
        block_ids[:, None] * (shard_order[:, None] == block_ids[None, :]).astype(jnp.int32), axis=0
    )
    own_rows = reorder_blocks(hidden_states, shard_order)
    attn_gain = reorder_blocks(gain_attn, shard_order)
    feed_gain = reorder_blocks(gain_ff, shard_order)
    final_gain = reorder_blocks(gain_final, shard_order)
    reward_head = reorder_blocks(w_reward, shard_order)
    row_count = own_rows.shape[0]
    row_start = lax.axis_index("tensor") * row_count

    qkv_full = lax.all_gather(
        jnp.concatenate([w_query, w_key, w_value], axis=1), "dp", axis=0, tiled=True
    )
    out_full = lax.all_gather(w_out, "dp", axis=1, tiled=True)
    gate_up_full = lax.all_gather(
        jnp.concatenate([w_gate, w_up], axis=1), "dp", axis=0, tiled=True
    )
    down_full = lax.all_gather(w_down, "dp", axis=1, tiled=True)

    normed = ring_gather(rms_norm(own_rows, attn_gain).astype(jnp.bfloat16))
    projected = jnp.dot(normed, qkv_full, preferred_element_type=jnp.float32).astype(jnp.bfloat16)

    heads = rel_bias.shape[1]
    relative = jnp.arange(4 * TILE, dtype=jnp.int32) - 2 * TILE
    onehot = (
        bucket_index(relative)[:, None]
        == jnp.arange(rel_bias.shape[0], dtype=jnp.int32)[None, :]
    ).astype(jnp.float32)
    bias_table = jnp.dot(onehot, rel_bias, precision=lax.Precision.HIGHEST).T
    bias_table = bias_table.reshape(heads // 2, 2, 4 * TILE)
    length = lengths[0]
    context = attention(lengths, projected, bias_table)

    attn_partial = jnp.dot(context, out_full, preferred_element_type=jnp.float32).astype(
        jnp.bfloat16
    )
    mid_own = own_rows + ring_scatter(attn_partial)
    mid_normed = ring_gather(rms_norm(mid_own, feed_gain).astype(jnp.bfloat16))
    hidden_width = w_gate.shape[1]
    gate_up = jnp.dot(mid_normed, gate_up_full, preferred_element_type=jnp.float32)
    activated = (
        jax.nn.gelu(gate_up[:, :hidden_width], approximate=True) * gate_up[:, hidden_width:]
    ).astype(jnp.bfloat16)
    feed_partial = jnp.dot(activated, down_full, preferred_element_type=jnp.float32).astype(
        jnp.bfloat16
    )
    output_rows = mid_own + ring_scatter(feed_partial)
    final_normed = rms_norm(output_rows, final_gain)
    token_score = jnp.dot(final_normed, reward_head, precision=lax.Precision.HIGHEST)
    positions = row_start + jnp.arange(row_count, dtype=jnp.int32)
    local_pool = jnp.sum(jnp.where(positions < length, token_score, 0.0))
    pooled_sum = total_over(jnp.reshape(local_pool, (1,)), "tensor")
    reward = pooled_sum / length.astype(jnp.float32)
    rollouts = lax.axis_size("dp") * lengths.shape[0]
    moments = total_over(jnp.concatenate([reward, reward * reward]), "dp")
    reward_mean = moments[0] / rollouts
    reward_var = moments[1] / rollouts - reward_mean * reward_mean
    normalized = (reward - reward_mean) / jnp.sqrt(reward_var + 1e-06)
    return (reorder_blocks(output_rows, inverse), normalized)


def put(ref, rows, value):
    ref[pl.ds(pl.multiple_of(rows, TILE // 2), value.shape[0]), :] = value


def slot_row(ids, shift, rows):
    return lax.rem(ids[1] + shift, 4) * rows


def true_block(order, ids, mask):
    return order[lax.bitwise_xor(ids[0], jnp.int32(mask))]


def spans(tiles):
    cut = (tiles + 1) // 2
    whole_blocks = [(mask, 0, tiles) for mask in range(6)]
    return whole_blocks + [(mask, *ends) for mask in (6, 7) for ends in ((0, cut), (cut, tiles))]


def fetch(order, ids, blocks, tiles, low, high, target, sem):
    for ref, (mask, first, last) in zip(blocks, spans(tiles)):
        start, stop = max(low, first), min(high, last)
        if start < stop:
            pltpu.make_async_copy(
                ref.at[pl.ds(start - first, stop - start)],
                target(true_block(order, ids, mask), start, stop - start),
                sem,
            ).start()


def into_rows(held, offset):
    block = held.shape[2]

    def target(where_to, start, count):
        rows = pl.ds(pl.multiple_of(where_to * block, block), block)
        return held.at[pl.ds(start - offset, count), rows, :]

    return target


def into_blocks(held, offset):
    return lambda where_to, start, count: held.at[where_to, pl.ds(start - offset, count)]


def arrived(part, sem):
    pltpu.make_async_copy(part, part, sem).wait()


def rms_kernel(x_ref, gain_ref, low_ref, high_ref):
    x = x_ref[...]
    scale = lax.rsqrt(jnp.mean(x * x, axis=-1, keepdims=True) + 1e-06)
    normed = (x * scale * gain_ref[...]).astype(jnp.bfloat16)
    half = low_ref.shape[0]
    low_ref[...] = normed[:half]
    high_ref[...] = normed[half:]


def pack_kernel(*refs):
    *sources, out = refs
    _, rows, wide = out.shape
    at = 0
    for s in sources:
        for i in range(s.shape[0] // rows):
            for j in range(s.shape[1] // wide):
                out[at] = s[i * rows : (i + 1) * rows, j * wide : (j + 1) * wide]
                at += 1


def project_kernel(order, ids, *refs):
    pieces = refs[:8]
    blocks = refs[8:18]
    out, x_all, w_all, sems = refs[18:]
    tiles, _, wide = w_all.shape
    stages = sems.shape[0]
    each = tiles // stages
    for g in range(stages):
        fetch(
            order, ids, blocks, tiles, g * each, (g + 1) * each, into_rows(w_all, 0), sems.at[g]
        )
    rows = pieces[0].shape[0]
    for slot, shift in enumerate((0, 3, 1, 2)):
        base = slot_row(ids, shift, 2 * rows)
        put(x_all, base, pieces[2 * slot][...])
        put(x_all, base + rows, pieces[2 * slot + 1][...])
    for j in range(tiles):
        if j % each == 0:
            arrived(w_all.at[pl.ds(j, each)], sems.at[j // each])
        out[:, j * wide : (j + 1) * wide] = jnp.dot(
            x_all[...], w_all[j], preferred_element_type=jnp.float32
        ).astype(out.dtype)


def out_kernel(order, ids, context, *refs):
    blocks = refs[:8]
    far_low, far_high, ahead_low, ahead_high, behind_low, behind_high, own = refs[8:15]
    x_all, w_all, sems = refs[15:]
    for mask in range(8):
        where_to = true_block(order, ids, mask)
        pltpu.make_async_copy(blocks[mask], w_all.at[where_to], sems.at[where_to]).start()
    rows = own.shape[0]
    half = rows // 2
    for slot, shift in enumerate((2, 1, 3, 0)):
        start = pl.multiple_of(slot_row(ids, shift, rows), rows)
        x_all[slot * rows : (slot + 1) * rows, :] = context[pl.ds(start, rows), :]
    wide = w_all.shape[2]

    @pl.loop(0, 8)
    def _(n):
        pltpu.make_async_copy(w_all.at[n], w_all.at[n], sems.at[n]).wait()
        columns = pl.ds(pl.multiple_of(n * wide, wide), wide)
        part = jnp.dot(x_all[...], w_all[n], preferred_element_type=jnp.float32).astype(own.dtype)
        for k, ref in enumerate(
            (far_low, far_high, ahead_low, ahead_high, behind_low, behind_high)
        ):
            ref[:, columns] = part[k * half : (k + 1) * half, :]
        own[:, columns] = part[3 * rows :, :]


def gelu(v):
    return 0.5 * v * (1.0 + jnp.tanh(0.7978845608028654 * (v + 0.044715 * (v * v * v))))


def feed_kernel(order, ids, *refs):
    pieces = refs[:8]
    blocks = refs[8:18]
    outs = refs[18:25]
    x_all, hidden, gate, up, down, sems = refs[25:]
    units, _, wide = gate.shape
    lead = 2
    for low, high, sem in ((0, lead, 0), (lead, units, 1)):
        fetch(order, ids, blocks, 3 * units, low, high, into_rows(gate, 0), sems.at[sem])
        fetch(
            order, ids, blocks, 3 * units, units + low, units + high,
            into_rows(up, units), sems.at[sem],
        )
    fetch(order, ids, blocks, 3 * units, 2 * units, 3 * units, into_blocks(down, 2 * units), sems.at[2])
    rows = pieces[0].shape[0]
    for k, piece in enumerate((6, 7, 4, 5, 2, 3, 0, 1)):
        x_all[k * rows : (k + 1) * rows, :] = pieces[piece][...]
    for j in range(units):
        if j in (0, lead):
            part = pl.ds(j, lead if j == 0 else units - lead)
            arrived(gate.at[part], sems.at[j // lead])
            arrived(up.at[part], sems.at[j // lead])
        gated = jnp.dot(x_all[...], gate[j], preferred_element_type=jnp.float32)
        upped = jnp.dot(x_all[...], up[j], preferred_element_type=jnp.float32)
        hidden[:, j * wide : (j + 1) * wide] = (gelu(gated) * upped).astype(hidden.dtype)
    arrived(down, sems.at[2])
    for n in range(8):
        part = jnp.dot(
            hidden[...], down[n].reshape(units * wide, wide), preferred_element_type=jnp.float32
        ).astype(outs[0].dtype)
        for k in range(6):
            outs[k][:, n * wide : (n + 1) * wide] = part[k * rows : (k + 1) * rows, :]
        outs[6][:, n * wide : (n + 1) * wide] = part[6 * rows :, :]


def residual(base, shares, half):
    own, before_low, before_high, after_low, after_high = shares
    low = base[:half] + (
        own[:half].astype(jnp.float32)
        + before_low[...].astype(jnp.float32)
        + after_low[...].astype(jnp.float32)
    )
    high = base[half:] + (
        own[half:].astype(jnp.float32)
        + before_high[...].astype(jnp.float32)
        + after_high[...].astype(jnp.float32)
    )
    return low, high


def mid_kernel(x_ref, *refs):
    shares, gain_ref, mid_ref, low_ref, high_ref = refs[:5], *refs[5:]
    half = low_ref.shape[0]
    for k, part in enumerate(residual(x_ref, shares, half)):
        mid_ref[k * half : (k + 1) * half, :] = part
        scale = lax.rsqrt(jnp.mean(part * part, axis=-1, keepdims=True) + 1e-06)
        (low_ref, high_ref)[k][...] = (part * scale * gain_ref[...]).astype(jnp.bfloat16)


def final_kernel(length, ids, x_ref, *refs):
    shares, gain_ref, head_ref, out_ref, pool_ref = refs[:5], *refs[5:]
    half = out_ref.shape[0] // 2
    pooled = jnp.zeros((1, 1), jnp.float32)
    for k, part in enumerate(residual(x_ref, shares, half)):
        out_ref[k * half : (k + 1) * half, :] = part
        scale = lax.rsqrt(jnp.mean(part * part, axis=-1, keepdims=True) + 1e-06)
        score = jnp.sum(part * scale * gain_ref[...] * head_ref[...], axis=-1, keepdims=True)
        position = (
            lax.broadcasted_iota(jnp.int32, (half, 1), 0) + ids[1] * (2 * half) + k * half
        )
        pooled = pooled + jnp.sum(
            jnp.where(position < length[0], score, 0.0), axis=0, keepdims=True
        )
    pool_ref[...] = jnp.broadcast_to(pooled, pool_ref.shape)


def whole(array):
    return pl.BlockSpec(array.shape, lambda *_: (0,) * len(array.shape))


def call(kernel, scalars, arrays, raw, outs, scratch, flops, moved):
    single = not isinstance(outs, (list, tuple))
    out_list = [outs] if single else list(outs)
    result = pl.pallas_call(
      kernel,
      out_shape=out_list,
      grid_spec=pltpu.PrefetchScalarGridSpec(
          num_scalar_prefetch=len(scalars),
          grid=(1,),
          in_specs=[whole(a) for a in arrays]
          + [pl.BlockSpec(memory_space=pl.ANY) for _ in raw],
          out_specs=[whole(o) for o in out_list],
          scratch_shapes=scratch,
      ),
      cost_estimate=pl.CostEstimate(flops=flops, bytes_accessed=moved, transcendentals=0),
    )(*scalars, *arrays, *raw)
    return result[0] if single else result


def shift_rows(block, step):
    return lax.ppermute(block, "tensor", ring_pairs(step))


def exchange(block, mask):
    return lax.ppermute(block, "dp", [(i, i ^ mask) for i in range(8)])


def plane_gather(block):
    held = {0: block}
    for mask in (2, 4, 6, 1):
        held[mask] = exchange(block, mask)
    for mask in (3, 5, 7):
        held[mask] = exchange(held[mask ^ 1], 1)
    return [held[mask] for mask in range(8)]


def plane_gather_split(block):
    cut = (block.shape[0] + 1) // 2
    held = {0: block}
    for mask in (2, 4, 1):
        held[mask] = exchange(block, mask)
    low = exchange(held[4][:cut], 2)
    high = exchange(held[2][cut:], 4)
    for mask in (3, 5):
        held[mask] = exchange(held[mask ^ 1], 1)
    pairs = [exchange(low, 1), exchange(high, 1)]
    return [held[mask] for mask in range(6)] + [low, high] + pairs


def half_gather(low, high):
    before_low = shift_rows(low, 1)
    after_high = shift_rows(high, -1)
    before_high = shift_rows(high, 1)
    after_low = shift_rows(low, -1)
    far_low = shift_rows(before_low, 1)
    far_high = shift_rows(after_high, -1)
    return [low, high, before_low, before_high, after_low, after_high, far_low, far_high]


def add_share(mine, received):
    return (mine.astype(jnp.float32) + received.astype(jnp.float32)).astype(mine.dtype)


def half_scatter(far_low, far_high, ahead_low, ahead_high, behind_low, behind_high, own):
    low = shift_rows(far_low, 1)
    high = shift_rows(far_high, -1)
    before_high = shift_rows(ahead_high, 1)
    after_low = shift_rows(behind_low, -1)
    before_low = shift_rows(add_share(ahead_low, low), 1)
    after_high = shift_rows(add_share(behind_high, high), -1)
    return [own, before_low, before_high, after_low, after_high]


def layer(
    hidden_states,
    lengths,
    shard_order,
    gain_attn,
    w_query,
    w_key,
    w_value,
    w_out,
    rel_bias,
    gain_ff,
    w_gate,
    w_up,
    w_down,
    gain_final,
    w_reward,
):
    bf16, f32 = jnp.bfloat16, jnp.float32
    shape = jax.ShapeDtypeStruct
    rows, width = hidden_states.shape
    half = rows // 2
    length_all = 4 * rows
    block = w_query.shape[0]
    inner = w_query.shape[1]
    hidden = w_gate.shape[1]
    ids = jnp.stack([lax.axis_index("dp"), lax.axis_index("tensor")]).astype(jnp.int32)
    half_bf = shape((half, width), bf16)
    row_bf = shape((rows, width), bf16)
    row_f32 = shape((rows, width), f32)

    qkv_own = call(
        pack_kernel, [], [w_query, w_key, w_value], [],
        shape((3 * inner // block, block, block), bf16), [], 2 * block * inner, 12 * block * inner,
    )
    low, high = call(
        rms_kernel, [], [hidden_states, gain_attn.reshape(1, width)], [],
        [half_bf, half_bf], [], 4 * rows * width, 6 * rows * width,
    )
    normed = half_gather(low, high)
    qkv = plane_gather_split(qkv_own)
    out_blocks = plane_gather(w_out)
    feed_own = call(
        pack_kernel, [], [w_gate, w_up, w_down], [],
        shape((3 * hidden // block, block, block), bf16), [], 2 * block * hidden, 12 * block * hidden,
    )
    feed = plane_gather_split(feed_own)

    projected = call(
        project_kernel, [shard_order, ids], normed, qkv,
        shape((length_all, 3 * inner), bf16),
        [
            pltpu.VMEM((length_all, width), bf16),
            pltpu.VMEM((3 * inner // block, width, block), bf16),
            pltpu.SemaphoreType.DMA((3,)),
        ],
        6 * length_all * width * inner, 6 * width * inner,
    )

    heads = rel_bias.shape[1]
    relative = jnp.arange(4 * TILE, dtype=jnp.int32) - 2 * TILE
    onehot = (
        bucket_index(relative)[:, None]
        == jnp.arange(rel_bias.shape[0], dtype=jnp.int32)[None, :]
    ).astype(f32)
    bias_table = jnp.dot(onehot, rel_bias, precision=lax.Precision.HIGHEST).T
    context = attention(lengths, projected, bias_table.reshape(heads // 2, 2, 4 * TILE))

    parts = call(
        out_kernel, [shard_order, ids], [context], out_blocks,
        [half_bf] * 6 + [row_bf],
        [
            pltpu.VMEM((length_all, inner), bf16),
            pltpu.VMEM((8, inner, block), bf16),
            pltpu.SemaphoreType.DMA((8,)),
        ],
        2 * length_all * width * inner, 2 * width * inner,
    )
    mid, low, high = call(
        mid_kernel, [],
        [hidden_states, *half_scatter(*parts), gain_ff.reshape(1, width)], [],
        [row_f32, half_bf, half_bf], [], 8 * rows * width, 16 * rows * width,
    )
    normed = half_gather(low, high)

    units = hidden // block
    parts = call(
        feed_kernel, [shard_order, ids], normed, feed, [half_bf] * 6 + [row_bf],
        [
            pltpu.VMEM((length_all, width), bf16),
            pltpu.VMEM((length_all, hidden), bf16),
            pltpu.VMEM((units, width, block), bf16),
            pltpu.VMEM((units, width, block), bf16),
            pltpu.VMEM((8, units, block, block), bf16),
            pltpu.SemaphoreType.DMA((3,)),
        ],
        6 * length_all * width * hidden, 6 * width * hidden,
    )
    shares = half_scatter(*parts)
    output_rows, pool = call(
        final_kernel, [lengths, ids],
        [mid, *shares, gain_final.reshape(1, width), w_reward.reshape(1, width)], [],
        [row_f32, shape((8, TILE), f32)], [], 8 * rows * width, 16 * rows * width,
    )
    total = pool
    for step in (1, 2):
        total = total + lax.ppermute(total, "tensor", [(i, i ^ step) for i in range(4)])
    reward = total / lengths[0].astype(f32)
    moments = jnp.where(lax.broadcasted_iota(jnp.int32, reward.shape, 0) == 0, reward, reward * reward)
    for mask in (1, 2, 4):
        moments = moments + exchange(moments, mask)
    reward_mean = moments[0, 0] / 8
    reward_var = moments[1, 0] / 8 - reward_mean * reward_mean
    normalized = (reward[0, 0] - reward_mean) / jnp.sqrt(reward_var + 1e-06)
    return (output_rows, jnp.reshape(normalized, (1,)))


def local_fast(*args):
    return layer(*args)


def solution(mesh):
    placed = (
        P(("dp", "tensor"), None),
        P("dp"),
        P(),
        P(),
        P("dp", "tensor"),
        P("dp", "tensor"),
        P("dp", "tensor"),
        P("tensor", "dp"),
        P(None, "tensor"),
        P(),
        P("dp", "tensor"),
        P("dp", "tensor"),
        P("tensor", "dp"),
        P(),
        P(),
    )
    fits = mesh.shape["dp"] == 8 and mesh.shape["tensor"] == 4
    return jax.shard_map(
        local_fast if fits else local_general,
        mesh=mesh,
        in_specs=placed,
        out_specs=(P(("dp", "tensor"), None), P("dp")),
        check_vma=False,
    )
```

```python
import functools
import math

import jax
import jax.numpy as jnp
from jax import lax
from jax.experimental import pallas as pl
from jax.experimental.pallas import tpu as pltpu
from jax.sharding import PartitionSpec as P


DK = 64
TILE = 128
GROUP = 512
SPARE = 4 << 20


bucket_edges = (12, 16, 23, 32, 46, 64, 91)


def bucket_index(relative):
    distance = jnp.abs(relative)
    bucket_low = jnp.minimum(distance, 8)
    for threshold in bucket_edges:
        bucket_low = bucket_low + (distance >= threshold).astype(jnp.int32)
    return jnp.where(relative > 0, 16, 0) + bucket_low


def rms_norm(values_in, weight_gain):
    return (
        values_in
        * lax.rsqrt(jnp.mean(values_in * values_in, axis=-1, keepdims=True) + 1e-06)
        * weight_gain
    )


def reorder_blocks(values_in, ordering):
    full_shape = values_in.shape
    blocks = values_in.reshape(
        full_shape[:-1] + (ordering.shape[0], full_shape[-1] // ordering.shape[0])
    )
    return jnp.take(blocks, ordering, axis=-2).reshape(full_shape)


def ring_pairs(step):
    size = lax.axis_size("tensor")
    return [(i, (i + step) % size) for i in range(size)]


def ring_gather(block):
    size = lax.axis_size("tensor")
    if size != 4:
        return lax.all_gather(block, "tensor", axis=0, tiled=True)
    rows = block.shape[0]
    half = rows // 2
    here = lax.axis_index("tensor")
    before = lax.ppermute(block, "tensor", ring_pairs(1))
    after = lax.ppermute(block, "tensor", ring_pairs(-1))
    far_low = lax.ppermute(before[:half], "tensor", ring_pairs(1))
    far_high = lax.ppermute(after[half:], "tensor", ring_pairs(-1))
    whole = jnp.zeros((size * rows,) + block.shape[1:], block.dtype)
    zero = jnp.int32(0)
    for piece, shift, offset in (
        (block, 0, 0),
        (before, 3, 0),
        (after, 1, 0),
        (far_low, 2, 0),
        (far_high, 2, half),
    ):
        start = ((here + shift) % size) * rows + offset
        whole = lax.dynamic_update_slice(whole, piece, (start, zero))
    return whole


def ring_scatter(partial):
    size = lax.axis_size("tensor")
    if size != 4:
        return lax.psum_scatter(partial, "tensor", scatter_dimension=0, tiled=True).astype(
            jnp.float32
        )
    rows = partial.shape[0] // size
    half = rows // 2
    here = lax.axis_index("tensor")

    def rows_of(shift):
        start = ((here + shift) % size) * rows
        return lax.dynamic_slice(partial, (start, jnp.int32(0)), (rows, partial.shape[1]))

    far = rows_of(2)
    low = lax.ppermute(far[:half], "tensor", ring_pairs(1))
    high = lax.ppermute(far[half:], "tensor", ring_pairs(-1))
    ahead = rows_of(1)
    behind = rows_of(3)
    ahead = jnp.concatenate(
        [
            (ahead[:half].astype(jnp.float32) + low.astype(jnp.float32)).astype(partial.dtype),
            ahead[half:],
        ]
    )
    behind = jnp.concatenate(
        [
            behind[:half],
            (behind[half:].astype(jnp.float32) + high.astype(jnp.float32)).astype(partial.dtype),
        ]
    )
    from_before = lax.ppermute(ahead, "tensor", ring_pairs(1))
    from_after = lax.ppermute(behind, "tensor", ring_pairs(-1))
    return (
        rows_of(0).astype(jnp.float32)
        + from_before.astype(jnp.float32)
        + from_after.astype(jnp.float32)
    )


def attention_kernel(length_ref, q_ref, k_ref, v_ref, bias_ref, o_ref):
    span, lanes = q_ref.shape
    blocks = span // TILE
    length = length_ref[0]
    keys = k_ref[...]
    values = v_ref[...]
    masked = jnp.where(lax.broadcasted_iota(jnp.int32, (1, span), 1) < length, 0.0, -1e30)
    first = lax.broadcasted_iota(jnp.int32, (1, lanes), 1) < DK
    one = jnp.ones_like(values)
    sums = []
    for head in range(2):
        table = bias_ref[pl.ds(2 * pl.program_id(0) + head, 1), :]
        near = pltpu.roll(
            jnp.broadcast_to(table, (TILE, 4 * TILE)), 0, 1, stride=1, stride_axis=0
        )
        own = first if head == 0 else jnp.logical_not(first)
        with_ones = jnp.where(own, values, one)
        far_left, far_right = table[:, 1:2], table[:, 4 * TILE - 1 :]
        heads = []
        for group in range(span // GROUP):
            queries = q_ref[group * GROUP : (group + 1) * GROUP, :]
            queries = jnp.where(own, queries, jnp.zeros_like(queries))
            scores = lax.dot_general(
                queries, keys, (((1,), (1,)), ((), ())), preferred_element_type=jnp.float32
            )
            soft = []
            for block in range(group * GROUP // TILE, (group + 1) * GROUP // TILE):
                row = block * TILE - group * GROUP
                pieces = []
                for other in range(blocks):
                    at = slice(other * TILE, (other + 1) * TILE)
                    delta = other - block
                    if abs(delta) > 1:
                        bias = masked[:, at] + (far_left if delta < 0 else far_right)
                    else:
                        bias = near[:, (delta + 2) * TILE : (delta + 3) * TILE] + masked[:, at]
                    pieces.append(scores[row : row + TILE, at] + bias)
                top = jnp.max(functools.reduce(jnp.maximum, pieces), axis=-1, keepdims=True)
                soft.append(
                    jnp.concatenate(
                        [jnp.exp(p - top).astype(jnp.bfloat16) for p in pieces], axis=1
                    )
                )
            heads.append(
                jnp.dot(
                    jnp.concatenate(soft, axis=0), with_ones, preferred_element_type=jnp.float32
                )
            )
        sums.append(heads)
    for group in range(span // GROUP):
        zero, last = sums[0][group], sums[1][group]
        total = pltpu.roll(jnp.where(first, last, zero), DK, 1)
        o_ref[group * GROUP : (group + 1) * GROUP, :] = (
            jnp.where(first, zero, last) / total
        ).astype(o_ref.dtype)


def attention(length, queries, keys, values, bias_table):
    span, inner = queries.shape
    pairs = inner // (2 * DK)
    return pl.pallas_call(
        attention_kernel,
        out_shape=jax.ShapeDtypeStruct((span, inner), jnp.bfloat16),
        grid_spec=pltpu.PrefetchScalarGridSpec(
            num_scalar_prefetch=1,
            grid=(pairs,),
            in_specs=[
                pl.BlockSpec((span, 2 * DK), lambda p, n: (0, p)),
                pl.BlockSpec((span, 2 * DK), lambda p, n: (0, p)),
                pl.BlockSpec((span, 2 * DK), lambda p, n: (0, p)),
                pl.BlockSpec(bias_table.shape, lambda p, n: (0, 0)),
            ],
            out_specs=pl.BlockSpec((span, 2 * DK), lambda p, n: (0, p)),
        ),
        cost_estimate=pl.CostEstimate(
            flops=16 * span * span * inner,
            bytes_accessed=8 * span * inner,
            transcendentals=span * span * inner // DK,
        ),
        compiler_params=pltpu.CompilerParams(vmem_limit_bytes=10 << 20),
        name="attention",
    )(length, queries, keys, values, bias_table)


def total_over(values_in, name):
    size = lax.axis_size(name)
    if size > 8:
        return lax.psum(values_in, name)
    total = values_in
    for step in range(1, size):
        total = total + lax.ppermute(
            values_in, name, [(i, (i + step) % size) for i in range(size)]
        )
    return total


def local_general(
    hidden_states,
    lengths,
    shard_order,
    gain_attn,
    w_query,
    w_key,
    w_value,
    w_out,
    rel_bias,
    gain_ff,
    w_gate,
    w_up,
    w_down,
    gain_final,
    w_reward,
):
    groups = shard_order.shape[0]
    block_ids = jnp.arange(groups, dtype=jnp.int32)
    inverse = jnp.sum(
        block_ids[:, None] * (shard_order[:, None] == block_ids[None, :]).astype(jnp.int32), axis=0
    )
    own_rows = reorder_blocks(hidden_states, shard_order)
    attn_gain = reorder_blocks(gain_attn, shard_order)
    feed_gain = reorder_blocks(gain_ff, shard_order)
    final_gain = reorder_blocks(gain_final, shard_order)
    reward_head = reorder_blocks(w_reward, shard_order)
    row_count = own_rows.shape[0]
    row_start = lax.axis_index("tensor") * row_count

    qkv_full = lax.all_gather(
        jnp.concatenate([w_query, w_key, w_value], axis=1), "dp", axis=0, tiled=True
    )
    out_full = lax.all_gather(w_out, "dp", axis=1, tiled=True)
    gate_up_full = lax.all_gather(
        jnp.concatenate([w_gate, w_up], axis=1), "dp", axis=0, tiled=True
    )
    down_full = lax.all_gather(w_down, "dp", axis=1, tiled=True)

    normed = ring_gather(rms_norm(own_rows, attn_gain).astype(jnp.bfloat16))
    projected = jnp.dot(normed, qkv_full, preferred_element_type=jnp.float32).astype(jnp.bfloat16)

    relative = jnp.arange(4 * TILE, dtype=jnp.int32) - 2 * TILE
    onehot = (
        bucket_index(relative)[:, None]
        == jnp.arange(rel_bias.shape[0], dtype=jnp.int32)[None, :]
    ).astype(jnp.float32)
    bias_table = jnp.dot(onehot, rel_bias, precision=lax.Precision.HIGHEST).T
    length = lengths[0]
    context = attention(lengths, *jnp.split(projected, 3, axis=1), bias_table)

    attn_partial = jnp.dot(context, out_full, preferred_element_type=jnp.float32).astype(
        jnp.bfloat16
    )
    mid_own = own_rows + ring_scatter(attn_partial)
    mid_normed = ring_gather(rms_norm(mid_own, feed_gain).astype(jnp.bfloat16))
    hidden_width = w_gate.shape[1]
    gate_up = jnp.dot(mid_normed, gate_up_full, preferred_element_type=jnp.float32)
    activated = (
        jax.nn.gelu(gate_up[:, :hidden_width], approximate=True) * gate_up[:, hidden_width:]
    ).astype(jnp.bfloat16)
    feed_partial = jnp.dot(activated, down_full, preferred_element_type=jnp.float32).astype(
        jnp.bfloat16
    )
    output_rows = mid_own + ring_scatter(feed_partial)
    final_normed = rms_norm(output_rows, final_gain)
    token_score = jnp.dot(final_normed, reward_head, precision=lax.Precision.HIGHEST)
    positions = row_start + jnp.arange(row_count, dtype=jnp.int32)
    local_pool = jnp.sum(jnp.where(positions < length, token_score, 0.0))
    pooled_sum = total_over(jnp.reshape(local_pool, (1,)), "tensor")
    reward = pooled_sum / length.astype(jnp.float32)
    rollouts = lax.axis_size("dp") * lengths.shape[0]
    moments = total_over(jnp.concatenate([reward, reward * reward]), "dp")
    reward_mean = moments[0] / rollouts
    reward_var = moments[1] / rollouts - reward_mean * reward_mean
    normalized = (reward - reward_mean) / jnp.sqrt(reward_var + 1e-06)
    return (reorder_blocks(output_rows, inverse), normalized)


def put(ref, rows, value):
    ref[pl.ds(pl.multiple_of(rows, TILE // 2), value.shape[0]), :] = value


def slot_row(ids, shift, rows):
    return lax.rem(ids[1] + shift, 4) * rows


def true_block(order, ids, mask):
    return order[lax.bitwise_xor(ids[0], jnp.int32(mask))]


def spans(tiles):
    cut = (tiles + 1) // 2
    whole_blocks = [(mask, 0, tiles) for mask in range(6)]
    return whole_blocks + [(mask, *ends) for mask in (6, 7) for ends in ((0, cut), (cut, tiles))]


def fetch(order, ids, blocks, tiles, low, high, target, sem):
    for ref, (mask, first, last) in zip(blocks, spans(tiles)):
        start, stop = max(low, first), min(high, last)
        if start < stop:
            pltpu.make_async_copy(
                ref.at[pl.ds(start - first, stop - start)],
                target(true_block(order, ids, mask), start, stop - start),
                sem,
            ).start()


def into_rows(held, offset):
    block = held.shape[2]

    def target(where_to, start, count):
        rows = pl.ds(pl.multiple_of(where_to * block, block), block)
        return held.at[pl.ds(start - offset, count), rows, :]

    return target


def into_blocks(held, offset):
    return lambda where_to, start, count: held.at[where_to, pl.ds(start - offset, count)]


def arrived(part, sem):
    pltpu.make_async_copy(part, part, sem).wait()


def rms_kernel(gain_ref, x_hbm, low_ref, high_ref, x_ref, sems):
    half = low_ref.shape[0]
    copies = [
        pltpu.make_async_copy(
            x_hbm.at[pl.ds(k * half, half)], x_ref.at[pl.ds(k * half, half)], sems.at[k]
        )
        for k in range(2)
    ]
    for copy in copies:
        copy.start()
    for k, out in enumerate((low_ref, high_ref)):
        copies[k].wait()
        x = x_ref[k * half : (k + 1) * half, :]
        scale = lax.rsqrt(jnp.mean(x * x, axis=-1, keepdims=True) + 1e-06)
        out[...] = (x * scale * gain_ref[...]).astype(jnp.bfloat16)


def pack_kernel(*refs):
    *sources, out, sem = refs
    _, rows, wide = out.shape
    at = 0
    for s in sources:
        for i in range(s.shape[0] // rows):
            for j in range(s.shape[1] // wide):
                pltpu.make_async_copy(
                    s.at[pl.ds(i * rows, rows), pl.ds(j * wide, wide)], out.at[at], sem.at[0]
                ).start()
                at += 1
    arrived(out, sem.at[0])


def project_kernel(order, ids, *refs):
    pieces = refs[:8]
    blocks = refs[8:18]
    *outs, x_all, w_all, sems = refs[18:]
    tiles, _, wide = w_all.shape
    stages = sems.shape[0]
    each = tiles // stages
    for g in range(stages):
        fetch(
            order, ids, blocks, tiles, g * each, (g + 1) * each, into_rows(w_all, 0), sems.at[g]
        )
    rows = pieces[0].shape[0]
    for slot, shift in enumerate((0, 3, 1, 2)):
        base = slot_row(ids, shift, 2 * rows)
        put(x_all, base, pieces[2 * slot][...])
        put(x_all, base + rows, pieces[2 * slot + 1][...])
    for j in range(tiles):
        if j % each == 0:
            arrived(w_all.at[pl.ds(j, each)], sems.at[j // each])
        out, column = outs[j // each], (j % each) * wide
        out[:, column : column + wide] = jnp.dot(
            x_all[...], w_all[j], preferred_element_type=jnp.float32
        ).astype(out.dtype)


def out_kernel(order, ids, context, *refs):
    blocks = refs[:8]
    far_low, far_high, ahead_low, ahead_high, behind_low, behind_high, own = refs[8:15]
    x_all, w_all, sems = refs[15:]
    wide = w_all.shape[2]
    for mask in range(8):
        where_to = true_block(order, ids, mask)
        at = pl.multiple_of(lax.rem(where_to, 2) * (wide // 2), wide // 2)
        pair = lax.div(where_to, 2)
        pltpu.make_async_copy(
            blocks[mask], w_all.at[pair, :, pl.ds(at, wide // 2)], sems.at[pair]
        ).start()
    rows = own.shape[0]
    half = rows // 2
    for slot, shift in enumerate((2, 1, 3, 0)):
        start = pl.multiple_of(slot_row(ids, shift, rows), rows)
        x_all[slot * rows : (slot + 1) * rows, :] = context[pl.ds(start, rows), :]

    @pl.loop(0, 4)
    def _(n):
        arrived(w_all.at[n], sems.at[n])
        columns = pl.ds(pl.multiple_of(n * wide, wide), wide)
        part = jnp.dot(x_all[...], w_all[n], preferred_element_type=jnp.float32).astype(own.dtype)
        for k, ref in enumerate(
            (far_low, far_high, ahead_low, ahead_high, behind_low, behind_high)
        ):
            ref[:, columns] = part[k * half : (k + 1) * half, :]
        own[:, columns] = part[3 * rows :, :]


def gelu(v):
    return 0.5 * v * (1.0 + jnp.tanh(0.7978845608028654 * (v + 0.044715 * (v * v * v))))


def gate_up(order, ids, blocks, rows, hidden, gate, up, sems):
    units, _, wide = gate.shape
    lead = 2
    for low, high, sem in ((0, lead, 0), (lead, units, 1)):
        fetch(order, ids, blocks, 3 * units, low, high, into_rows(gate, 0), sems.at[sem])
        fetch(
            order, ids, blocks, 3 * units, units + low, units + high,
            into_rows(up, units), sems.at[sem],
        )
    yield
    for j in range(units):
        if j in (0, lead):
            part = pl.ds(j, lead if j == 0 else units - lead)
            arrived(gate.at[part], sems.at[j // lead])
            arrived(up.at[part], sems.at[j // lead])
        gated = jnp.dot(rows[...], gate[j], preferred_element_type=jnp.float32)
        upped = jnp.dot(rows[...], up[j], preferred_element_type=jnp.float32)
        hidden[:, j * wide : (j + 1) * wide] = (gelu(gated) * upped).astype(hidden.dtype)


def near_kernel(order, ids, *refs):
    pieces, blocks = refs[:6], refs[6:16]
    hidden, x_all, gate, up, sems = refs[16:]
    work = gate_up(order, ids, blocks, x_all, hidden, gate, up, sems)
    next(work)
    rows = pieces[0].shape[0]
    for k, piece in enumerate((4, 5, 2, 3, 0, 1)):
        x_all[k * rows : (k + 1) * rows, :] = pieces[piece][...]
    for _ in work:
        pass


def feed_kernel(order, ids, near, *refs):
    pieces, blocks = refs[:2], refs[2:12]
    outs = refs[12:19]
    x_all, hidden, gate, up, down, sems = refs[19:]
    units, _, wide = gate.shape
    rows = pieces[0].shape[0]
    work = gate_up(order, ids, blocks, x_all, hidden, gate, up, sems)
    next(work)
    fetch(order, ids, blocks, 3 * units, 2 * units, 3 * units, into_blocks(down, 2 * units), sems.at[2])
    for k in range(2):
        x_all[k * rows : (k + 1) * rows, :] = pieces[k][...]
    for _ in work:
        pass
    arrived(down, sems.at[2])
    for n in range(8):
        columns = slice(n * wide, (n + 1) * wide)
        weights = down[n].reshape(units * wide, wide)
        far = jnp.dot(hidden[...], weights, preferred_element_type=jnp.float32)
        rest = jnp.dot(near[...], weights, preferred_element_type=jnp.float32)
        far, rest = far.astype(outs[0].dtype), rest.astype(outs[0].dtype)
        for k in range(2):
            outs[k][:, columns] = far[k * rows : (k + 1) * rows, :]
        for k in range(4):
            outs[2 + k][:, columns] = rest[k * rows : (k + 1) * rows, :]
        outs[6][:, columns] = rest[4 * rows :, :]


def residual(base, shares, half):
    own, before_low, before_high, after_low, after_high = shares
    low = base[:half] + (
        own[:half].astype(jnp.float32)
        + before_low[...].astype(jnp.float32)
        + after_low[...].astype(jnp.float32)
    )
    high = base[half:] + (
        own[half:].astype(jnp.float32)
        + before_high[...].astype(jnp.float32)
        + after_high[...].astype(jnp.float32)
    )
    return low, high


def mid_kernel(x_ref, *refs):
    shares, gain_ref, mid_ref, low_ref, high_ref = refs[:5], *refs[5:]
    half = low_ref.shape[0]
    for k, part in enumerate(residual(x_ref, shares, half)):
        mid_ref[k * half : (k + 1) * half, :] = part
        scale = lax.rsqrt(jnp.mean(part * part, axis=-1, keepdims=True) + 1e-06)
        (low_ref, high_ref)[k][...] = (part * scale * gain_ref[...]).astype(jnp.bfloat16)


def final_kernel(length, ids, x_ref, *refs):
    shares, gain_ref, head_ref, out_ref, pool_ref = refs[:5], *refs[5:]
    half = out_ref.shape[0] // 2
    pooled = jnp.zeros((1, 1), jnp.float32)
    for k, part in enumerate(residual(x_ref, shares, half)):
        out_ref[k * half : (k + 1) * half, :] = part
        scale = lax.rsqrt(jnp.mean(part * part, axis=-1, keepdims=True) + 1e-06)
        score = jnp.sum(part * scale * gain_ref[...] * head_ref[...], axis=-1, keepdims=True)
        position = (
            lax.broadcasted_iota(jnp.int32, (half, 1), 0) + ids[1] * (2 * half) + k * half
        )
        pooled = pooled + jnp.sum(
            jnp.where(position < length[0], score, 0.0), axis=0, keepdims=True
        )
    pool_ref[...] = jnp.broadcast_to(pooled, pool_ref.shape)


def whole(array):
    return pl.BlockSpec(array.shape, lambda *_: (0,) * len(array.shape))


def room(array):
    sized = hasattr(array, "dtype") and array.dtype in (jnp.bfloat16, jnp.float32)
    return math.prod(array.shape) * jnp.dtype(array.dtype).itemsize if sized else 0


def call(kernel, scalars, arrays, raw, outs, scratch, flops, moved):
    single = not isinstance(outs, (list, tuple))
    out_list = [outs] if single else list(outs)
    held = 2 * sum(map(room, [*arrays, *out_list])) + sum(map(room, scratch))
    result = pl.pallas_call(
      kernel,
      out_shape=out_list,
      grid_spec=pltpu.PrefetchScalarGridSpec(
          num_scalar_prefetch=len(scalars),
          grid=(1,),
          in_specs=[whole(a) for a in arrays]
          + [pl.BlockSpec(memory_space=pl.ANY) for _ in raw],
          out_specs=[whole(o) for o in out_list],
          scratch_shapes=scratch,
      ),
      cost_estimate=pl.CostEstimate(flops=flops, bytes_accessed=moved, transcendentals=0),
      compiler_params=pltpu.CompilerParams(vmem_limit_bytes=held + SPARE),
    )(*scalars, *arrays, *raw)
    return result[0] if single else result


def shift_rows(block, step):
    return lax.ppermute(block, "tensor", ring_pairs(step))


def exchange(block, mask):
    return lax.ppermute(block, "dp", [(i, i ^ mask) for i in range(8)])


def plane_gather(block):
    held = {0: block}
    for mask in (2, 4, 6, 1):
        held[mask] = exchange(block, mask)
    for mask in (3, 5, 7):
        held[mask] = exchange(held[mask ^ 1], 1)
    return [held[mask] for mask in range(8)]


def plane_gather_split(block):
    cut = (block.shape[0] + 1) // 2
    held = {0: block}
    for mask in (2, 4, 1):
        held[mask] = exchange(block, mask)
    low = exchange(held[4][:cut], 2)
    high = exchange(held[2][cut:], 4)
    for mask in (3, 5):
        held[mask] = exchange(held[mask ^ 1], 1)
    pairs = [exchange(low, 1), exchange(high, 1)]
    return [held[mask] for mask in range(6)] + [low, high] + pairs


def half_gather(low, high):
    before_low = shift_rows(low, 1)
    after_high = shift_rows(high, -1)
    before_high = shift_rows(high, 1)
    after_low = shift_rows(low, -1)
    far_low = shift_rows(before_low, 1)
    far_high = shift_rows(after_high, -1)
    return [low, high, before_low, before_high, after_low, after_high, far_low, far_high]


def add_share(mine, received):
    return (mine.astype(jnp.float32) + received.astype(jnp.float32)).astype(mine.dtype)


def half_scatter(far_low, far_high, ahead_low, ahead_high, behind_low, behind_high, own):
    low = shift_rows(far_low, 1)
    high = shift_rows(far_high, -1)
    before_high = shift_rows(ahead_high, 1)
    after_low = shift_rows(behind_low, -1)
    before_low = shift_rows(add_share(ahead_low, low), 1)
    after_high = shift_rows(add_share(behind_high, high), -1)
    return [own, before_low, before_high, after_low, after_high]


def layer(
    hidden_states,
    lengths,
    shard_order,
    gain_attn,
    w_query,
    w_key,
    w_value,
    w_out,
    rel_bias,
    gain_ff,
    w_gate,
    w_up,
    w_down,
    gain_final,
    w_reward,
):
    bf16, f32 = jnp.bfloat16, jnp.float32
    shape = jax.ShapeDtypeStruct
    rows, width = hidden_states.shape
    half = rows // 2
    length_all = 4 * rows
    block = w_query.shape[0]
    inner = w_query.shape[1]
    hidden = w_gate.shape[1]
    ids = jnp.stack([lax.axis_index("dp"), lax.axis_index("tensor")]).astype(jnp.int32)
    half_bf = shape((half, width), bf16)
    row_bf = shape((rows, width), bf16)
    row_f32 = shape((rows, width), f32)

    qkv_own = call(
        pack_kernel, [], [], [w_query, w_key, w_value],
        shape((3 * inner // block, block, block), bf16), [pltpu.SemaphoreType.DMA((1,))], 2 * block * inner, 12 * block * inner,
    )
    low, high = call(
        rms_kernel, [], [gain_attn.reshape(1, width)], [hidden_states],
        [half_bf, half_bf],
        [pltpu.VMEM((rows, width), f32), pltpu.SemaphoreType.DMA((2,))], 4 * rows * width, 6 * rows * width,
    )
    normed = half_gather(low, high)
    qkv = plane_gather_split(qkv_own)
    out_blocks = plane_gather(w_out)
    feed_own = call(
        pack_kernel, [], [], [w_gate, w_up, w_down],
        shape((3 * hidden // block, block, block), bf16), [pltpu.SemaphoreType.DMA((1,))], 2 * block * hidden, 12 * block * hidden,
    )
    feed = plane_gather_split(feed_own)

    queries, keys, values = call(
        project_kernel, [shard_order, ids], normed, qkv,
        [shape((length_all, inner), bf16)] * 3,
        [
            pltpu.VMEM((length_all, width), bf16),
            pltpu.VMEM((3 * inner // block, width, block), bf16),
            pltpu.SemaphoreType.DMA((3,)),
        ],
        6 * length_all * width * inner, 6 * width * inner,
    )

    relative = jnp.arange(4 * TILE, dtype=jnp.int32) - 2 * TILE
    onehot = (
        bucket_index(relative)[:, None]
        == jnp.arange(rel_bias.shape[0], dtype=jnp.int32)[None, :]
    ).astype(f32)
    bias_table = jnp.dot(onehot, rel_bias, precision=lax.Precision.HIGHEST).T
    context = attention(
        lengths, queries, keys, values, bias_table
    )

    parts = call(
        out_kernel, [shard_order, ids], [context], out_blocks,
        [half_bf] * 6 + [row_bf],
        [
            pltpu.VMEM((length_all, inner), bf16),
            pltpu.VMEM((4, inner, 2 * block), bf16),
            pltpu.SemaphoreType.DMA((4,)),
        ],
        2 * length_all * width * inner, 2 * width * inner,
    )
    mid, low, high = call(
        mid_kernel, [],
        [hidden_states, *half_scatter(*parts), gain_ff.reshape(1, width)], [],
        [row_f32, half_bf, half_bf], [], 8 * rows * width, 16 * rows * width,
    )
    normed = half_gather(low, high)

    units = hidden // block
    weights = pltpu.VMEM((units, width, block), bf16)
    near = call(
        near_kernel, [shard_order, ids], normed[:6], feed,
        shape((3 * rows, hidden), bf16),
        [pltpu.VMEM((3 * rows, width), bf16), weights, weights, pltpu.SemaphoreType.DMA((2,))],
        12 * rows * width * hidden, 4 * width * hidden,
    )
    parts = call(
        feed_kernel, [shard_order, ids], [near, *normed[6:]], feed,
        [half_bf] * 6 + [row_bf],
        [
            pltpu.VMEM((rows, width), bf16),
            pltpu.VMEM((rows, hidden), bf16),
            weights,
            weights,
            pltpu.VMEM((8, units, block, block), bf16),
            pltpu.SemaphoreType.DMA((3,)),
        ],
        12 * rows * width * hidden, 6 * width * hidden,
    )
    shares = half_scatter(*parts)
    output_rows, pool = call(
        final_kernel, [lengths, ids],
        [mid, *shares, gain_final.reshape(1, width), w_reward.reshape(1, width)], [],
        [row_f32, shape((8, TILE), f32)], [], 8 * rows * width, 16 * rows * width,
    )
    total = pool
    for step in (1, 2, 3):
        total = total + lax.ppermute(pool, "tensor", [(i, i ^ step) for i in range(4)])
    reward = total / lengths[0].astype(f32)
    moments = jnp.where(lax.broadcasted_iota(jnp.int32, reward.shape, 0) == 0, reward, reward * reward)
    for mask in (1, 2, 4):
        moments = moments + exchange(moments, mask)
    reward_mean = moments[0, 0] / 8
    reward_var = moments[1, 0] / 8 - reward_mean * reward_mean
    normalized = (reward[0, 0] - reward_mean) / jnp.sqrt(reward_var + 1e-06)
    return (output_rows, jnp.reshape(normalized, (1,)))


def local_fast(*args):
    return layer(*args)


def solution(mesh):
    placed = (
        P(("dp", "tensor"), None),
        P("dp"),
        P(),
        P(),
        P("dp", "tensor"),
        P("dp", "tensor"),
        P("dp", "tensor"),
        P("tensor", "dp"),
        P(None, "tensor"),
        P(),
        P("dp", "tensor"),
        P("dp", "tensor"),
        P("tensor", "dp"),
        P(),
        P(),
    )
    fits = mesh.shape["dp"] == 8 and mesh.shape["tensor"] == 4
    return jax.shard_map(
        local_fast if fits else local_general,
        mesh=mesh,
        in_specs=placed,
        out_specs=(P(("dp", "tensor"), None), P("dp")),
        check_vma=False,
    )
```

```python
import functools
import math

import jax
import jax.numpy as jnp
from jax import lax
from jax.experimental import pallas as pl
from jax.experimental.pallas import tpu as pltpu
from jax.sharding import PartitionSpec as P


DK = 64
TILE = 128
GROUP = 512
SPARE = 4 << 20


bucket_edges = (12, 16, 23, 32, 46, 64, 91)


def bucket_index(relative):
    distance = jnp.abs(relative)
    bucket_low = jnp.minimum(distance, 8)
    for threshold in bucket_edges:
        bucket_low = bucket_low + (distance >= threshold).astype(jnp.int32)
    return jnp.where(relative > 0, 16, 0) + bucket_low


def rms_norm(values_in, weight_gain):
    return (
        values_in
        * lax.rsqrt(jnp.mean(values_in * values_in, axis=-1, keepdims=True) + 1e-06)
        * weight_gain
    )


def reorder_blocks(values_in, ordering):
    full_shape = values_in.shape
    blocks = values_in.reshape(
        full_shape[:-1] + (ordering.shape[0], full_shape[-1] // ordering.shape[0])
    )
    return jnp.take(blocks, ordering, axis=-2).reshape(full_shape)


def ring_pairs(step):
    size = lax.axis_size("tensor")
    return [(i, (i + step) % size) for i in range(size)]


def ring_gather(block):
    size = lax.axis_size("tensor")
    if size != 4:
        return lax.all_gather(block, "tensor", axis=0, tiled=True)
    rows = block.shape[0]
    half = rows // 2
    here = lax.axis_index("tensor")
    before = lax.ppermute(block, "tensor", ring_pairs(1))
    after = lax.ppermute(block, "tensor", ring_pairs(-1))
    far_low = lax.ppermute(before[:half], "tensor", ring_pairs(1))
    far_high = lax.ppermute(after[half:], "tensor", ring_pairs(-1))
    whole = jnp.zeros((size * rows,) + block.shape[1:], block.dtype)
    zero = jnp.int32(0)
    for piece, shift, offset in (
        (block, 0, 0),
        (before, 3, 0),
        (after, 1, 0),
        (far_low, 2, 0),
        (far_high, 2, half),
    ):
        start = ((here + shift) % size) * rows + offset
        whole = lax.dynamic_update_slice(whole, piece, (start, zero))
    return whole


def ring_scatter(partial):
    size = lax.axis_size("tensor")
    if size != 4:
        return lax.psum_scatter(partial, "tensor", scatter_dimension=0, tiled=True).astype(
            jnp.float32
        )
    rows = partial.shape[0] // size
    half = rows // 2
    here = lax.axis_index("tensor")

    def rows_of(shift):
        start = ((here + shift) % size) * rows
        return lax.dynamic_slice(partial, (start, jnp.int32(0)), (rows, partial.shape[1]))

    far = rows_of(2)
    low = lax.ppermute(far[:half], "tensor", ring_pairs(1))
    high = lax.ppermute(far[half:], "tensor", ring_pairs(-1))
    ahead = rows_of(1)
    behind = rows_of(3)
    ahead = jnp.concatenate(
        [
            (ahead[:half].astype(jnp.float32) + low.astype(jnp.float32)).astype(partial.dtype),
            ahead[half:],
        ]
    )
    behind = jnp.concatenate(
        [
            behind[:half],
            (behind[half:].astype(jnp.float32) + high.astype(jnp.float32)).astype(partial.dtype),
        ]
    )
    from_before = lax.ppermute(ahead, "tensor", ring_pairs(1))
    from_after = lax.ppermute(behind, "tensor", ring_pairs(-1))
    return (
        rows_of(0).astype(jnp.float32)
        + from_before.astype(jnp.float32)
        + from_after.astype(jnp.float32)
    )


def attention_kernel(length_ref, q_ref, k_ref, v_ref, bias_ref, o_ref):
    span, lanes = q_ref.shape
    blocks = span // TILE
    length = length_ref[0]
    keys = k_ref[...]
    values = v_ref[...]
    masked = jnp.where(lax.broadcasted_iota(jnp.int32, (1, span), 1) < length, 0.0, -1e30)
    first = lax.broadcasted_iota(jnp.int32, (1, lanes), 1) < DK
    one = jnp.ones_like(values)
    sums = []
    for head in range(2):
        table = bias_ref[pl.ds(2 * pl.program_id(0) + head, 1), :]
        near = pltpu.roll(
            jnp.broadcast_to(table, (TILE, 4 * TILE)), 0, 1, stride=1, stride_axis=0
        )
        own = first if head == 0 else jnp.logical_not(first)
        with_ones = jnp.where(own, values, one)
        far_left, far_right = table[:, 1:2], table[:, 4 * TILE - 1 :]
        heads = []
        for group in range(span // GROUP):
            queries = q_ref[group * GROUP : (group + 1) * GROUP, :]
            queries = jnp.where(own, queries, jnp.zeros_like(queries))
            scores = lax.dot_general(
                queries, keys, (((1,), (1,)), ((), ())), preferred_element_type=jnp.float32
            )
            soft = []
            for block in range(group * GROUP // TILE, (group + 1) * GROUP // TILE):
                row = block * TILE - group * GROUP
                pieces = []
                for other in range(blocks):
                    at = slice(other * TILE, (other + 1) * TILE)
                    delta = other - block
                    if abs(delta) > 1:
                        bias = masked[:, at] + (far_left if delta < 0 else far_right)
                    else:
                        bias = near[:, (delta + 2) * TILE : (delta + 3) * TILE] + masked[:, at]
                    pieces.append(scores[row : row + TILE, at] + bias)
                top = jnp.max(functools.reduce(jnp.maximum, pieces), axis=-1, keepdims=True)
                soft.append(
                    jnp.concatenate(
                        [jnp.exp(p - top).astype(jnp.bfloat16) for p in pieces], axis=1
                    )
                )
            heads.append(
                jnp.dot(
                    jnp.concatenate(soft, axis=0), with_ones, preferred_element_type=jnp.float32
                )
            )
        sums.append(heads)
    for group in range(span // GROUP):
        zero, last = sums[0][group], sums[1][group]
        total = pltpu.roll(jnp.where(first, last, zero), DK, 1)
        o_ref[group * GROUP : (group + 1) * GROUP, :] = (
            jnp.where(first, zero, last) / total
        ).astype(o_ref.dtype)


def attention(length, queries, keys, values, bias_table):
    span, inner = queries.shape
    pairs = inner // (2 * DK)
    return pl.pallas_call(
        attention_kernel,
        out_shape=jax.ShapeDtypeStruct((span, inner), jnp.bfloat16),
        grid_spec=pltpu.PrefetchScalarGridSpec(
            num_scalar_prefetch=1,
            grid=(pairs,),
            in_specs=[
                pl.BlockSpec((span, 2 * DK), lambda p, n: (0, p)),
                pl.BlockSpec((span, 2 * DK), lambda p, n: (0, p)),
                pl.BlockSpec((span, 2 * DK), lambda p, n: (0, p)),
                pl.BlockSpec(bias_table.shape, lambda p, n: (0, 0)),
            ],
            out_specs=pl.BlockSpec((span, 2 * DK), lambda p, n: (0, p)),
        ),
        cost_estimate=pl.CostEstimate(
            flops=16 * span * span * inner,
            bytes_accessed=8 * span * inner,
            transcendentals=span * span * inner // DK,
        ),
        compiler_params=pltpu.CompilerParams(vmem_limit_bytes=10 << 20),
        name="attention",
    )(length, queries, keys, values, bias_table)


def total_over(values_in, name):
    size = lax.axis_size(name)
    if size > 8:
        return lax.psum(values_in, name)
    total = values_in
    for step in range(1, size):
        total = total + lax.ppermute(
            values_in, name, [(i, (i + step) % size) for i in range(size)]
        )
    return total


def local_general(
    hidden_states,
    lengths,
    shard_order,
    gain_attn,
    w_query,
    w_key,
    w_value,
    w_out,
    rel_bias,
    gain_ff,
    w_gate,
    w_up,
    w_down,
    gain_final,
    w_reward,
):
    groups = shard_order.shape[0]
    block_ids = jnp.arange(groups, dtype=jnp.int32)
    inverse = jnp.sum(
        block_ids[:, None] * (shard_order[:, None] == block_ids[None, :]).astype(jnp.int32), axis=0
    )
    own_rows = reorder_blocks(hidden_states, shard_order)
    attn_gain = reorder_blocks(gain_attn, shard_order)
    feed_gain = reorder_blocks(gain_ff, shard_order)
    final_gain = reorder_blocks(gain_final, shard_order)
    reward_head = reorder_blocks(w_reward, shard_order)
    row_count = own_rows.shape[0]
    row_start = lax.axis_index("tensor") * row_count

    qkv_full = lax.all_gather(
        jnp.concatenate([w_query, w_key, w_value], axis=1), "dp", axis=0, tiled=True
    )
    out_full = lax.all_gather(w_out, "dp", axis=1, tiled=True)
    gate_up_full = lax.all_gather(
        jnp.concatenate([w_gate, w_up], axis=1), "dp", axis=0, tiled=True
    )
    down_full = lax.all_gather(w_down, "dp", axis=1, tiled=True)

    normed = ring_gather(rms_norm(own_rows, attn_gain).astype(jnp.bfloat16))
    projected = jnp.dot(normed, qkv_full, preferred_element_type=jnp.float32).astype(jnp.bfloat16)

    relative = jnp.arange(4 * TILE, dtype=jnp.int32) - 2 * TILE
    onehot = (
        bucket_index(relative)[:, None]
        == jnp.arange(rel_bias.shape[0], dtype=jnp.int32)[None, :]
    ).astype(jnp.float32)
    bias_table = jnp.dot(onehot, rel_bias, precision=lax.Precision.HIGHEST).T
    length = lengths[0]
    context = attention(lengths, *jnp.split(projected, 3, axis=1), bias_table)

    attn_partial = jnp.dot(context, out_full, preferred_element_type=jnp.float32).astype(
        jnp.bfloat16
    )
    mid_own = own_rows + ring_scatter(attn_partial)
    mid_normed = ring_gather(rms_norm(mid_own, feed_gain).astype(jnp.bfloat16))
    hidden_width = w_gate.shape[1]
    gate_up = jnp.dot(mid_normed, gate_up_full, preferred_element_type=jnp.float32)
    activated = (
        jax.nn.gelu(gate_up[:, :hidden_width], approximate=True) * gate_up[:, hidden_width:]
    ).astype(jnp.bfloat16)
    feed_partial = jnp.dot(activated, down_full, preferred_element_type=jnp.float32).astype(
        jnp.bfloat16
    )
    output_rows = mid_own + ring_scatter(feed_partial)
    final_normed = rms_norm(output_rows, final_gain)
    token_score = jnp.dot(final_normed, reward_head, precision=lax.Precision.HIGHEST)
    positions = row_start + jnp.arange(row_count, dtype=jnp.int32)
    local_pool = jnp.sum(jnp.where(positions < length, token_score, 0.0))
    pooled_sum = total_over(jnp.reshape(local_pool, (1,)), "tensor")
    reward = pooled_sum / length.astype(jnp.float32)
    rollouts = lax.axis_size("dp") * lengths.shape[0]
    moments = total_over(jnp.concatenate([reward, reward * reward]), "dp")
    reward_mean = moments[0] / rollouts
    reward_var = moments[1] / rollouts - reward_mean * reward_mean
    normalized = (reward - reward_mean) / jnp.sqrt(reward_var + 1e-06)
    return (reorder_blocks(output_rows, inverse), normalized)


def put(ref, rows, value):
    ref[pl.ds(pl.multiple_of(rows, TILE // 2), value.shape[0]), :] = value


def slot_row(ids, shift, rows):
    return lax.rem(ids[1] + shift, 4) * rows


def true_block(order, ids, mask):
    return order[lax.bitwise_xor(ids[0], jnp.int32(mask))]


def spans(tiles):
    cut = (tiles + 1) // 2
    whole_blocks = [(mask, 0, tiles) for mask in range(6)]
    return whole_blocks + [(mask, *ends) for mask in (6, 7) for ends in ((0, cut), (cut, tiles))]


def fetch(order, ids, blocks, tiles, low, high, target, sem):
    for ref, (mask, first, last) in zip(blocks, spans(tiles)):
        start, stop = max(low, first), min(high, last)
        if start < stop:
            pltpu.make_async_copy(
                ref.at[pl.ds(start - first, stop - start)],
                target(true_block(order, ids, mask), start, stop - start),
                sem,
            ).start()


def into_rows(held, offset):
    block = held.shape[2]

    def target(where_to, start, count):
        rows = pl.ds(pl.multiple_of(where_to * block, block), block)
        return held.at[pl.ds(start - offset, count), rows, :]

    return target


def into_blocks(held, offset):
    return lambda where_to, start, count: held.at[where_to, pl.ds(start - offset, count)]


def arrived(part, sem):
    pltpu.make_async_copy(part, part, sem).wait()


def rms_kernel(gain_ref, x_hbm, low_ref, high_ref, x_ref, sems):
    half = low_ref.shape[0]
    copies = [
        pltpu.make_async_copy(
            x_hbm.at[pl.ds(k * half, half)], x_ref.at[pl.ds(k * half, half)], sems.at[k]
        )
        for k in range(2)
    ]
    for copy in copies:
        copy.start()
    for k, out in enumerate((low_ref, high_ref)):
        copies[k].wait()
        x = x_ref[k * half : (k + 1) * half, :]
        scale = lax.rsqrt(jnp.mean(x * x, axis=-1, keepdims=True) + 1e-06)
        out[...] = (x * scale * gain_ref[...]).astype(jnp.bfloat16)


def pack_kernel(*refs):
    *sources, out, sem = refs
    _, rows, wide = out.shape
    at = 0
    for s in sources:
        for i in range(s.shape[0] // rows):
            for j in range(s.shape[1] // wide):
                pltpu.make_async_copy(
                    s.at[pl.ds(i * rows, rows), pl.ds(j * wide, wide)], out.at[at], sem.at[0]
                ).start()
                at += 1
    arrived(out, sem.at[0])


def project_kernel(order, ids, *refs):
    pieces = refs[:8]
    blocks = refs[8:18]
    *outs, x_all, w_all, sems = refs[18:]
    tiles, _, wide = w_all.shape
    stages = sems.shape[0]
    each = tiles // stages
    for g in range(stages):
        fetch(
            order, ids, blocks, tiles, g * each, (g + 1) * each, into_rows(w_all, 0), sems.at[g]
        )
    rows = pieces[0].shape[0]
    for slot, shift in enumerate((0, 3, 1, 2)):
        base = slot_row(ids, shift, 2 * rows)
        put(x_all, base, pieces[2 * slot][...])
        put(x_all, base + rows, pieces[2 * slot + 1][...])
    for j in range(tiles):
        if j % each == 0:
            arrived(w_all.at[pl.ds(j, each)], sems.at[j // each])
        out, column = outs[j // each], (j % each) * wide
        out[:, column : column + wide] = jnp.dot(
            x_all[...], w_all[j], preferred_element_type=jnp.float32
        ).astype(out.dtype)


def out_kernel(order, ids, context, *refs):
    blocks = refs[:8]
    far_low, far_high, ahead_low, ahead_high, behind_low, behind_high, own = refs[8:15]
    x_all, w_all, sems = refs[15:]
    wide = w_all.shape[2]
    for mask in range(8):
        where_to = true_block(order, ids, mask)
        at = pl.multiple_of(lax.rem(where_to, 2) * (wide // 2), wide // 2)
        pair = lax.div(where_to, 2)
        pltpu.make_async_copy(
            blocks[mask], w_all.at[pair, :, pl.ds(at, wide // 2)], sems.at[pair]
        ).start()
    rows = own.shape[0]
    half = rows // 2
    for slot, shift in enumerate((2, 1, 3, 0)):
        start = pl.multiple_of(slot_row(ids, shift, rows), rows)
        x_all[slot * rows : (slot + 1) * rows, :] = context[pl.ds(start, rows), :]

    @pl.loop(0, 4)
    def _(n):
        arrived(w_all.at[n], sems.at[n])
        columns = pl.ds(pl.multiple_of(n * wide, wide), wide)
        part = jnp.dot(x_all[...], w_all[n], preferred_element_type=jnp.float32).astype(own.dtype)
        for k, ref in enumerate(
            (far_low, far_high, ahead_low, ahead_high, behind_low, behind_high)
        ):
            ref[:, columns] = part[k * half : (k + 1) * half, :]
        own[:, columns] = part[3 * rows :, :]


def gelu(v):
    return 0.5 * v * (1.0 + jnp.tanh(0.7978845608028654 * (v + 0.044715 * (v * v * v))))


def gate_up(order, ids, blocks, rows, hidden, gate, up, sems):
    units, _, wide = gate.shape
    lead = 2
    for low, high, sem in ((0, lead, 0), (lead, units, 1)):
        fetch(order, ids, blocks, 3 * units, low, high, into_rows(gate, 0), sems.at[sem])
        fetch(
            order, ids, blocks, 3 * units, units + low, units + high,
            into_rows(up, units), sems.at[sem],
        )
    yield
    for j in range(units):
        if j in (0, lead):
            part = pl.ds(j, lead if j == 0 else units - lead)
            arrived(gate.at[part], sems.at[j // lead])
            arrived(up.at[part], sems.at[j // lead])
        gated = jnp.dot(rows[...], gate[j], preferred_element_type=jnp.float32)
        upped = jnp.dot(rows[...], up[j], preferred_element_type=jnp.float32)
        hidden[:, j * wide : (j + 1) * wide] = (gelu(gated) * upped).astype(hidden.dtype)


def near_kernel(order, ids, *refs):
    pieces, blocks = refs[:6], refs[6:16]
    hidden, x_all, gate, up, sems = refs[16:]
    work = gate_up(order, ids, blocks, x_all, hidden, gate, up, sems)
    next(work)
    rows = pieces[0].shape[0]
    for k, piece in enumerate((4, 5, 2, 3, 0, 1)):
        x_all[k * rows : (k + 1) * rows, :] = pieces[piece][...]
    for _ in work:
        pass


def feed_kernel(order, ids, near, *refs):
    pieces, blocks = refs[:2], refs[2:12]
    outs = refs[12:19]
    x_all, hidden, gate, up, down, sems = refs[19:]
    units, _, wide = gate.shape
    rows = pieces[0].shape[0]
    work = gate_up(order, ids, blocks, x_all, hidden, gate, up, sems)
    next(work)
    fetch(order, ids, blocks, 3 * units, 2 * units, 3 * units, into_blocks(down, 2 * units), sems.at[2])
    for k in range(2):
        x_all[k * rows : (k + 1) * rows, :] = pieces[k][...]
    for _ in work:
        pass
    arrived(down, sems.at[2])
    for n in range(8):
        columns = slice(n * wide, (n + 1) * wide)
        weights = down[n].reshape(units * wide, wide)
        far = jnp.dot(hidden[...], weights, preferred_element_type=jnp.float32)
        rest = jnp.dot(near[...], weights, preferred_element_type=jnp.float32)
        far, rest = far.astype(outs[0].dtype), rest.astype(outs[0].dtype)
        for k in range(2):
            outs[k][:, columns] = far[k * rows : (k + 1) * rows, :]
        for k in range(4):
            outs[2 + k][:, columns] = rest[k * rows : (k + 1) * rows, :]
        outs[6][:, columns] = rest[4 * rows :, :]


def residual(base, shares, half):
    own, before_low, before_high, after_low, after_high = shares
    low = base[:half] + (
        own[:half].astype(jnp.float32)
        + before_low[...].astype(jnp.float32)
        + after_low[...].astype(jnp.float32)
    )
    high = base[half:] + (
        own[half:].astype(jnp.float32)
        + before_high[...].astype(jnp.float32)
        + after_high[...].astype(jnp.float32)
    )
    return low, high


def mid_kernel(x_ref, *refs):
    shares, gain_ref, mid_ref, low_ref, high_ref = refs[:5], *refs[5:]
    half = low_ref.shape[0]
    for k, part in enumerate(residual(x_ref, shares, half)):
        mid_ref[k * half : (k + 1) * half, :] = part
        scale = lax.rsqrt(jnp.mean(part * part, axis=-1, keepdims=True) + 1e-06)
        (low_ref, high_ref)[k][...] = (part * scale * gain_ref[...]).astype(jnp.bfloat16)


def final_kernel(length, ids, x_ref, *refs):
    shares, gain_ref, head_ref, out_ref, pool_ref = refs[:5], *refs[5:]
    half = out_ref.shape[0] // 2
    pooled = jnp.zeros((1, 1), jnp.float32)
    for k, part in enumerate(residual(x_ref, shares, half)):
        out_ref[k * half : (k + 1) * half, :] = part
        scale = lax.rsqrt(jnp.mean(part * part, axis=-1, keepdims=True) + 1e-06)
        score = jnp.sum(part * scale * gain_ref[...] * head_ref[...], axis=-1, keepdims=True)
        position = (
            lax.broadcasted_iota(jnp.int32, (half, 1), 0) + ids[1] * (2 * half) + k * half
        )
        pooled = pooled + jnp.sum(
            jnp.where(position < length[0], score, 0.0), axis=0, keepdims=True
        )
    pool_ref[...] = jnp.broadcast_to(pooled, pool_ref.shape)


def standard_kernel(reward, first, second, third, fourth, out):
    moments = (first[...] + second[...] + third[...] + fourth[...]) / 8
    mean, square = moments[0:1, 0:1], moments[1:2, 0:1]
    out[...] = (reward[0:1, 0:1] - mean) / jnp.sqrt(square - mean * mean + 1e-06)


def whole(array):
    return pl.BlockSpec(array.shape, lambda *_: (0,) * len(array.shape))


def room(array):
    sized = hasattr(array, "dtype") and array.dtype in (jnp.bfloat16, jnp.float32)
    return math.prod(array.shape) * jnp.dtype(array.dtype).itemsize if sized else 0


def call(kernel, scalars, arrays, raw, outs, scratch, flops, moved):
    single = not isinstance(outs, (list, tuple))
    out_list = [outs] if single else list(outs)
    held = 2 * sum(map(room, [*arrays, *out_list])) + sum(map(room, scratch))
    result = pl.pallas_call(
      kernel,
      out_shape=out_list,
      grid_spec=pltpu.PrefetchScalarGridSpec(
          num_scalar_prefetch=len(scalars),
          grid=(1,),
          in_specs=[whole(a) for a in arrays]
          + [pl.BlockSpec(memory_space=pl.ANY) for _ in raw],
          out_specs=[whole(o) for o in out_list],
          scratch_shapes=scratch,
      ),
      cost_estimate=pl.CostEstimate(flops=flops, bytes_accessed=moved, transcendentals=0),
      compiler_params=pltpu.CompilerParams(vmem_limit_bytes=held + SPARE),
    )(*scalars, *arrays, *raw)
    return result[0] if single else result


def shift_rows(block, step):
    return lax.ppermute(block, "tensor", ring_pairs(step))


def exchange(block, mask):
    return lax.ppermute(block, "dp", [(i, i ^ mask) for i in range(8)])


def plane_gather(block):
    held = {0: block}
    for mask in (2, 4, 6, 1):
        held[mask] = exchange(block, mask)
    for mask in (3, 5, 7):
        held[mask] = exchange(held[mask ^ 1], 1)
    return [held[mask] for mask in range(8)]


def plane_gather_split(block):
    cut = (block.shape[0] + 1) // 2
    held = {0: block}
    for mask in (2, 4, 1):
        held[mask] = exchange(block, mask)
    high = exchange(held[2][cut:], 4)
    low = exchange(held[4][:cut], 2)
    for mask in (3, 5):
        held[mask] = exchange(held[mask ^ 1], 1)
    pairs = [exchange(low, 1), exchange(high, 1)]
    return [held[mask] for mask in range(6)] + [low, high] + pairs


def half_gather(low, high):
    before_low = shift_rows(low, 1)
    after_high = shift_rows(high, -1)
    before_high = shift_rows(high, 1)
    after_low = shift_rows(low, -1)
    far_low = shift_rows(before_low, 1)
    far_high = shift_rows(after_high, -1)
    return [low, high, before_low, before_high, after_low, after_high, far_low, far_high]


def add_share(mine, received):
    return (mine.astype(jnp.float32) + received.astype(jnp.float32)).astype(mine.dtype)


def half_scatter(far_low, far_high, ahead_low, ahead_high, behind_low, behind_high, own):
    low = shift_rows(far_low, 1)
    high = shift_rows(far_high, -1)
    before_high = shift_rows(ahead_high, 1)
    after_low = shift_rows(behind_low, -1)
    before_low = shift_rows(add_share(ahead_low, low), 1)
    after_high = shift_rows(add_share(behind_high, high), -1)
    return [own, before_low, before_high, after_low, after_high]


def layer(
    hidden_states,
    lengths,
    shard_order,
    gain_attn,
    w_query,
    w_key,
    w_value,
    w_out,
    rel_bias,
    gain_ff,
    w_gate,
    w_up,
    w_down,
    gain_final,
    w_reward,
):
    bf16, f32 = jnp.bfloat16, jnp.float32
    shape = jax.ShapeDtypeStruct
    rows, width = hidden_states.shape
    half = rows // 2
    length_all = 4 * rows
    block = w_query.shape[0]
    inner = w_query.shape[1]
    hidden = w_gate.shape[1]
    ids = jnp.stack([lax.axis_index("dp"), lax.axis_index("tensor")]).astype(jnp.int32)
    half_bf = shape((half, width), bf16)
    row_bf = shape((rows, width), bf16)
    row_f32 = shape((rows, width), f32)

    qkv_own = call(
        pack_kernel, [], [], [w_query, w_key, w_value],
        shape((3 * inner // block, block, block), bf16), [pltpu.SemaphoreType.DMA((1,))], 2 * block * inner, 12 * block * inner,
    )
    low, high = call(
        rms_kernel, [], [gain_attn.reshape(1, width)], [hidden_states],
        [half_bf, half_bf],
        [pltpu.VMEM((rows, width), f32), pltpu.SemaphoreType.DMA((2,))], 4 * rows * width, 6 * rows * width,
    )
    normed = half_gather(low, high)
    qkv = plane_gather_split(qkv_own)
    out_blocks = plane_gather(w_out)
    feed_own = call(
        pack_kernel, [], [], [w_gate, w_up, w_down],
        shape((3 * hidden // block, block, block), bf16), [pltpu.SemaphoreType.DMA((1,))], 2 * block * hidden, 12 * block * hidden,
    )
    feed = plane_gather_split(feed_own)

    queries, keys, values = call(
        project_kernel, [shard_order, ids], normed, qkv,
        [shape((length_all, inner), bf16)] * 3,
        [
            pltpu.VMEM((length_all, width), bf16),
            pltpu.VMEM((3 * inner // block, width, block), bf16),
            pltpu.SemaphoreType.DMA((3,)),
        ],
        6 * length_all * width * inner, 6 * width * inner,
    )

    relative = jnp.arange(4 * TILE, dtype=jnp.int32) - 2 * TILE
    onehot = (
        bucket_index(relative)[:, None]
        == jnp.arange(rel_bias.shape[0], dtype=jnp.int32)[None, :]
    ).astype(f32)
    bias_table = jnp.dot(onehot, rel_bias, precision=lax.Precision.HIGHEST).T
    context = attention(
        lengths, queries, keys, values, bias_table
    )

    parts = call(
        out_kernel, [shard_order, ids], [context], out_blocks,
        [half_bf] * 6 + [row_bf],
        [
            pltpu.VMEM((length_all, inner), bf16),
            pltpu.VMEM((4, inner, 2 * block), bf16),
            pltpu.SemaphoreType.DMA((4,)),
        ],
        2 * length_all * width * inner, 2 * width * inner,
    )
    mid, low, high = call(
        mid_kernel, [],
        [hidden_states, *half_scatter(*parts), gain_ff.reshape(1, width)], [],
        [row_f32, half_bf, half_bf], [], 8 * rows * width, 16 * rows * width,
    )
    normed = half_gather(low, high)

    units = hidden // block
    weights = pltpu.VMEM((units, width, block), bf16)
    near = call(
        near_kernel, [shard_order, ids], normed[:6], feed,
        shape((3 * rows, hidden), bf16),
        [pltpu.VMEM((3 * rows, width), bf16), weights, weights, pltpu.SemaphoreType.DMA((2,))],
        12 * rows * width * hidden, 4 * width * hidden,
    )
    parts = call(
        feed_kernel, [shard_order, ids], [near, *normed[6:]], feed,
        [half_bf] * 6 + [row_bf],
        [
            pltpu.VMEM((rows, width), bf16),
            pltpu.VMEM((rows, hidden), bf16),
            weights,
            weights,
            pltpu.VMEM((8, units, block, block), bf16),
            pltpu.SemaphoreType.DMA((3,)),
        ],
        12 * rows * width * hidden, 6 * width * hidden,
    )
    shares = half_scatter(*parts)
    output_rows, pool = call(
        final_kernel, [lengths, ids],
        [mid, *shares, gain_final.reshape(1, width), w_reward.reshape(1, width)], [],
        [row_f32, shape((8, TILE), f32)], [], 8 * rows * width, 16 * rows * width,
    )
    total = pool
    for step in (1, 2, 3):
        total = total + lax.ppermute(pool, "tensor", [(i, i ^ step) for i in range(4)])
    reward = total / lengths[0].astype(f32)
    moments = jnp.where(lax.broadcasted_iota(jnp.int32, reward.shape, 0) == 0, reward, reward * reward)
    moments = moments + exchange(moments, 1)
    sums = [moments] + [exchange(moments, mask) for mask in (2, 4, 6)]
    normalized = call(standard_kernel, [], [reward, *sums], [], shape((1, 1), f32), [], 8192, 20480)
    return (output_rows, jnp.reshape(normalized, (1,)))


def local_fast(*args):
    return layer(*args)


def solution(mesh):
    placed = (
        P(("dp", "tensor"), None),
        P("dp"),
        P(),
        P(),
        P("dp", "tensor"),
        P("dp", "tensor"),
        P("dp", "tensor"),
        P("tensor", "dp"),
        P(None, "tensor"),
        P(),
        P("dp", "tensor"),
        P("dp", "tensor"),
        P("tensor", "dp"),
        P(),
        P(),
    )
    fits = mesh.shape["dp"] == 8 and mesh.shape["tensor"] == 4
    return jax.shard_map(
        local_fast if fits else local_general,
        mesh=mesh,
        in_specs=placed,
        out_specs=(P(("dp", "tensor"), None), P("dp")),
        check_vma=False,
    )
```
